32 devices in a mesh: lat: 8 (over y, x, core), lon: 4 (over z).
Axes of the slice: x: 2, y: 2, z: 4, core: 2. Of those that a mesh axis runs over, the one named last changes fastest.
Arguments:
- coeffs_old: float32 [640, 2, 3, 50, 640], P(('lat', 'lon')), may hold values from -0.16 to 0.16
- noise: bfloat16 [640, 2, 3, 50, 640], P(('lat', 'lon')), may hold values from -6 to 6
- legendre: float32 [640, 640, 640], P(('lat', 'lon')), may hold values from -0.25 to 0.25
- decay: float32 [3], replicated, may hold values from 0.3 to 0.97
- amplitude: float32 [3, 640], replicated, may hold values from 0.005 to 0.05
- wavenumber_of_slot: int32 [640], replicated, may hold values from 0 to 639, as said below
- lat_order: int32 [640], replicated, may hold values from 0 to 639, each once
Outputs:
- coeffs_new: float32 [640, 2, 3, 50, 640], P(('lat', 'lon'))
- pattern: float32 [640, 50, 1280], P(('lat', 'lon'))
The draws below stay inside these ranges and needn't reach their ends.
Inputs may be any that keep to these rules, and one draw needn't show every extreme that they name: `wavenumber_of_slot`: every wavenumber fills exactly one slot; the sums of the wavenumbers of one device's 20 slots differ between devices by less than 32. `lat_order`: every latitude stands in exactly one row.
All inputs are finite; a program needn't handle non-finite values.
Results may differ from the reference program's by a relative error of at most 0.0003.
Values sent between devices are 32-bit elements; how exact they have to be, the bound alone decides.
A program may use at most 192 MiB of HBM per device.

```python
import math
import jax
import jax.numpy as jnp
from jax import lax

M = 640
LAT = 640
LON = 1280
SCALES = 3
MEMBERS = 50
SLOT_DEV = 20


def draw_wavenumber_of_slot(key, part):
    devices_all = M // SLOT_DEV
    position = jax.random.permutation(jax.random.fold_in(key, 11), devices_all).astype(jnp.int32)
    rounds = jnp.arange(SLOT_DEV, dtype=jnp.int32)
    dealt = jnp.where(rounds[None, :] % 2 == 0, position[:, None], devices_all - 1 - position[:, None])
    table = rounds[None, :] * devices_all + dealt
    return table.reshape(-1).astype(jnp.int32)


def shard_levels(stream_key, shape, cuts, low, high):
    def one(dim, blocks):
        steps = jax.random.uniform(jax.random.fold_in(jax.random.fold_in(stream_key, 6), dim), (blocks,), jnp.float32, low / len(cuts), high / len(cuts))
        return jnp.repeat(jnp.exp(steps), shape[dim] // blocks).reshape((-1,) + (1,) * (len(shape) - dim - 1))

    loudness = one(*cuts[0])
    for cut in cuts[1:]:
        loudness = loudness * one(*cut)
    return loudness


def scatter_about(own_key, dims, scale, bound, shards=(), kind=jnp.bfloat16):
    result = scale * jax.random.normal(own_key, dims, jnp.float32)
    if shards:
        result = result * shard_levels(own_key, dims, shards, -0.22, 0.18)
    return jnp.clip(result, -bound, bound).astype(kind)


def setup_inputs(seed: int = 0) -> dict:
    arg_keys = jax.random.split(jax.random.key(seed), 8)
    coeffs_old = scatter_about(arg_keys[0], (M, 2, SCALES, MEMBERS, M), 0.02, 0.16, ((0, 32),), jnp.float32)
    noise = scatter_about(arg_keys[1], (M, 2, SCALES, MEMBERS, M), 1.0, 6.0, ((0, 32),))
    legendre = scatter_about(arg_keys[2], (M, LAT, M), M ** -0.5, 0.25, ((0, 32),), jnp.float32)
    decay = jnp.clip(jax.random.uniform(arg_keys[3], (SCALES,), jnp.float32, 0.3, 0.97), 0.3, 0.97)
    amplitude = jnp.clip(jnp.exp(jax.random.uniform(arg_keys[4], (SCALES, M), jnp.float32, math.log(0.005), math.log(0.05))), 0.005, 0.05)
    wavenumber_of_slot = draw_wavenumber_of_slot(jax.random.fold_in(arg_keys[7], 71), 0)
    lat_order = jax.random.permutation(arg_keys[6], LAT).astype(jnp.int32)
    return {"coeffs_old": coeffs_old, "noise": noise, "legendre": legendre, "decay": decay, "amplitude": amplitude, "wavenumber_of_slot": wavenumber_of_slot, "lat_order": lat_order}


def evolve(coeffs_old, noise, decay, amplitude, waves):
    width = coeffs_old.shape[4]
    offsets = lax.broadcasted_iota(jnp.int32, (waves.shape[0], width), 1)
    live = waves[:, None] + offsets < width
    padded = jnp.concatenate([amplitude, jnp.zeros_like(amplitude)], axis=1)
    spread = jax.vmap(lambda wave: lax.dynamic_slice_in_dim(padded, wave, width, 1))(waves)
    factor = jnp.sqrt(1.0 - decay * decay)
    fresh = decay[None, None, :, None, None] * coeffs_old + (spread * factor[None, :, None])[:, None, :, None, :] * noise.astype(jnp.float32)
    return jnp.where(live[:, None, None, None, :], fresh, jnp.zeros_like(fresh))

def reference(coeffs_old, noise, legendre, decay, amplitude, wavenumber_of_slot, lat_order):
    waves = wavenumber_of_slot.astype(jnp.int32)
    coeffs_new = evolve(coeffs_old, noise, decay, amplitude, waves)

    def per_slot(pair):
        coeff, basis = pair
        return jnp.einsum('rkej,lj->rel', coeff, basis, precision=lax.Precision.HIGHEST)
    field = lax.map(per_slot, (coeffs_new, legendre))
    real_part = jnp.zeros((M,) + field.shape[2:], field.dtype).at[waves].set(field[:, 0])
    imag_part = jnp.zeros((M,) + field.shape[2:], field.dtype).at[waves].set(field[:, 1])
    positive = jnp.arange(M, dtype=jnp.int32)[:, None, None] > 0
    imag_part = jnp.where(positive, imag_part, jnp.zeros_like(imag_part))
    real_part = jnp.take(real_part, lat_order.astype(jnp.int32), axis=2)
    imag_part = jnp.take(imag_part, lat_order.astype(jnp.int32), axis=2)
    spectrum = real_part + 1j * imag_part
    grid = jnp.fft.irfft(spectrum, n=LON, axis=0) * LON
    pattern = jnp.transpose(grid, (2, 1, 0))
    return (coeffs_new, pattern)
```

```python
import functools

import jax
import jax.numpy as jnp
from jax import lax
from jax.experimental import pallas as pl
from jax.experimental.pallas import tpu as pltpu
from jax.sharding import PartitionSpec as P

TWO_PI = 6.283185307179586
LANES = 128
HALF = 64
MESH = pl.DeviceIdType.MESH


def round_up(size, unit):
    return -(-size // unit) * unit


def group_size(slots):
    return 4 if slots % 4 == 0 else slots


def split(x):
    high = x.astype(jnp.bfloat16)
    return high, (x - high.astype(jnp.float32)).astype(jnp.bfloat16)


def legendre_product(basis, both):
    contract = (((1,), (1,)), ((), ()))
    basis_high, basis_low = split(basis)
    first = lax.dot_general(basis_high, both, contract, preferred_element_type=jnp.float32)
    second = lax.dot_general(basis_low, both[:LANES], contract, preferred_element_type=jnp.float32)
    return first[:, :LANES] + first[:, LANES:] + second


def pack_group(order_ref, field, store, devices, lat_dev, members, rows, wide):
    lane = lax.broadcasted_iota(jnp.int32, (rows, LANES), 1)

    def pack(device, carry):
        tiles = [jnp.zeros((rows, LANES), jnp.float32) for _ in range(wide // LANES)]
        for q in range(lat_dev):
            piece = field[order_ref[device * lat_dev + q]]
            start = members * q
            offset = start % LANES
            if offset:
                piece = pltpu.roll(piece, offset, axis=1)
            tile = start // LANES
            tiles[tile] = jnp.where((lane >= offset) & (lane < offset + members), piece, tiles[tile])
            if offset + members > LANES:
                tiles[tile + 1] = jnp.where(lane < offset + members - LANES, piece, tiles[tile + 1])
        for index, tile in enumerate(tiles):
            store(device, index, tile)
        return carry

    lax.fori_loop(0, devices, pack, 0)


def update_kernel(group, order_ref, waves_ref, decay_ref, old_ref, noise_ref, basis_ref, spread_ref, new_ref, both_ref, send_ref, weights, field):
    step = pl.program_id(0)
    scales, members, parts, width = old_ref.shape[1:]
    devices, rows, wide = send_ref.shape
    lat_dev = order_ref.shape[0] // devices

    @pl.when(step == 0)
    def _():
        weights[...] = jnp.zeros_like(weights)
        if 2 * group < rows:
            field[...] = jnp.zeros_like(field)

    wave = waves_ref[step]
    live = lax.broadcasted_iota(jnp.int32, (8, width), 1) + wave < width
    shifted = jnp.where(live, pltpu.roll(spread_ref[...], width - wave, axis=1), 0.0)
    total = None
    for scale in range(scales):
        keep = jnp.where(live[:1], decay_ref[scale], 0.0).reshape(1, 1, width)
        fresh = shifted[scale : scale + 1, :].reshape(1, 1, width)
        value = keep * old_ref[0, scale] + fresh * noise_ref[0, scale].astype(jnp.float32)
        new_ref[0, scale] = value
        total = value if total is None else total + value
    for part in range(parts):
        weights[part * HALF : part * HALF + members, :] = total[:, part, :]
    high, low = split(weights[...])
    both_ref[0, :LANES] = high
    both_ref[0, LANES:] = low

    @pl.when(step < group)
    def _():
        product = legendre_product(basis_ref[0], both_ref[0])
        other = pltpu.roll(product, HALF, axis=1)
        for index in range(group):

            @pl.when(step == index)
            def _(index=index):
                field[:, 2 * index, :] = product
                field[:, 2 * index + 1, :] = other

    @pl.when(step == group - 1)
    def _():
        def store(device, index, tile):
            send_ref[device, :, index * LANES : (index + 1) * LANES] = tile

        pack_group(order_ref, field, store, devices, lat_dev, members, rows, wide)


def update(old, noise, legendre, spread, decay, waves, lat_order, devices, rows, wide, group):
    slots, scales, members, parts, width = old.shape
    lats = legendre.shape[1]

    def slot5(i, *_):
        return (i, 0, 0, 0, 0)

    spec = pltpu.PrefetchScalarGridSpec(
        num_scalar_prefetch=3,
        grid=(slots,),
        in_specs=[
            pl.BlockSpec((1, scales, members, parts, width), slot5),
            pl.BlockSpec((1, scales, members, parts, width), slot5),
            pl.BlockSpec((1, lats, width), lambda i, *_: (jnp.minimum(i, group - 1), 0, 0)),
            pl.BlockSpec((8, width), lambda i, *_: (0, 0)),
        ],
        out_specs=[
            pl.BlockSpec((1, scales, members, parts, width), slot5),
            pl.BlockSpec((1, 2 * LANES, width), lambda i, *_: (i, 0, 0)),
            pl.BlockSpec((devices, rows, wide), lambda i, *_: (0, 0, 0)),
        ],
        scratch_shapes=[
            pltpu.VMEM((LANES, width), jnp.float32),
            pltpu.VMEM((lats, rows, LANES), jnp.float32),
        ],
    )
    return pl.pallas_call(
        functools.partial(update_kernel, group),
        grid_spec=spec,
        out_shape=[
            jax.ShapeDtypeStruct(old.shape, jnp.float32),
            jax.ShapeDtypeStruct((slots, 2 * LANES, width), jnp.bfloat16),
            jax.ShapeDtypeStruct((devices, rows, wide), jnp.float32),
        ],
        compiler_params=pltpu.CompilerParams(dimension_semantics=("arbitrary",)),
        name="update",
    )(lat_order, waves, decay, old, noise, legendre, spread)


def exchange_kernel(
    group, members, order_ref, first_ref, both_hbm, basis_hbm, phase_ref, out_ref,
    basis, both, field, send, recv, turned, left, table, load_sem, own_sem, send_sem, recv_sem,
):
    lat_size, lon_size = lax.axis_size("lat"), lax.axis_size("lon")
    devices = lat_size * lon_size
    me = lax.axis_index("lat") * lon_size + lax.axis_index("lon")
    slots, lats = basis_hbm.shape[0], basis_hbm.shape[1]
    groups, _, rows, wide = recv.shape
    lat_dev = lats // devices
    padded, length = out_ref.shape[1], out_ref.shape[2]
    depth = devices * rows

    def peer(k):
        other = lax.rem(me + k, devices)
        return other, (other // lon_size, lax.rem(other, lon_size))

    barrier = pltpu.get_barrier_semaphore()

    def greet(k, carry):
        pl.semaphore_signal(barrier, inc=1, device_id=peer(k)[1], device_id_type=MESH)
        return carry

    lax.fori_loop(1, devices, greet, 0)

    def loads(slot):
        side = lax.rem(slot, 2)
        return (
            pltpu.make_async_copy(basis_hbm.at[slot], basis.at[side], load_sem.at[0, side]),
            pltpu.make_async_copy(both_hbm.at[slot], both.at[side], load_sem.at[1, side]),
        )

    if slots > group:
        for copy in loads(group):
            copy.start()
    left[...] = jnp.zeros_like(left)
    if 2 * group < rows:
        field[...] = jnp.zeros_like(field)
    pl.semaphore_wait(barrier, devices - 1)

    def send_group(source, index):
        def one(k, carry):
            other, where = peer(k)
            pltpu.make_async_remote_copy(
                src_ref=source.at[other],
                dst_ref=recv.at[index, me],
                send_sem=send_sem.at[index],
                recv_sem=recv_sem.at[index],
                device_id=where,
                device_id_type=MESH,
            ).start()
            return carry

        lax.fori_loop(1, devices, one, 0)
        pltpu.make_async_copy(source.at[me], recv.at[index, me], own_sem.at[index]).start()

    send_group(first_ref, 0)

    def transform(index, carry):
        for inner in range(group):
            slot = index * group + inner
            for copy in loads(slot):
                copy.wait()

            @pl.when(slot + 1 < slots)
            def _():
                for copy in loads(slot + 1):
                    copy.start()

            side = lax.rem(slot, 2)
            product = legendre_product(basis[side], both[side])
            field[:, 2 * inner, :] = product
            field[:, 2 * inner + 1, :] = pltpu.roll(product, HALF, axis=1)

        def store(device, tile_index, tile):
            send[index - 1, device, :, tile_index * LANES : (tile_index + 1) * LANES] = tile

        pack_group(order_ref, field, store, devices, lat_dev, members, rows, wide)
        send_group(send.at[index - 1], index)
        return carry

    lax.fori_loop(1, groups, transform, 0)

    def make_table(index):
        wave = phase_ref[pl.ds(pl.multiple_of(index * depth, depth), depth), :]
        lane = lax.broadcasted_iota(jnp.int32, wave.shape, 1).astype(jnp.float32)
        row = lax.broadcasted_iota(jnp.int32, wave.shape, 0)
        quarter = jnp.where(lax.rem(row, 2) == 0, 0.0, TWO_PI / 4)
        weight = jnp.where(wave == 0.0, 1.0, 2.0)

        def angle(steps):
            turns = jnp.floor(steps * (1.0 / length))
            return (steps - turns * length) * (TWO_PI / length)

        base = angle(wave * lane) + quarter
        cosine, sine = weight * jnp.cos(base), weight * jnp.sin(base)
        for block in range(length // LANES):
            if block == 0:
                value = cosine
            else:
                value = jnp.cos(angle(wave * float(LANES * block))) * cosine - jnp.sin(angle(wave * float(LANES * block))) * sine
            high, low = split(value)
            span = slice(block * LANES, (block + 1) * LANES)
            table[:depth, span] = high
            table[depth : 2 * depth, span] = high
            table[2 * depth :, span] = low

    def synthesis(index, carry):
        make_table(index)
        pltpu.make_async_copy(recv.at[index, pl.ds(0, devices - 1)], recv.at[index, pl.ds(0, devices - 1)], recv_sem.at[index]).wait()
        pltpu.make_async_copy(recv.at[index, 0], recv.at[index, 0], own_sem.at[index]).wait()
        turned[...] = recv[index].reshape(depth, wide).T
        for q in range(lat_dev):
            high, low = split(turned[members * q : members * (q + 1), :])
            left[q, :members, :depth] = high.astype(jnp.float32)
            left[q, :members, depth:] = low.astype(jnp.float32)
        values = left[...].reshape(lat_dev * padded, 2 * depth).astype(jnp.bfloat16)
        chunk = 2 * LANES

        def columns(n, carry):
            span = pl.ds(pl.multiple_of(n * chunk, chunk), chunk)
            part = jnp.dot(values, table[: 2 * depth, span], preferred_element_type=jnp.float32)
            part += jnp.dot(values[:, :depth], table[2 * depth :, span], preferred_element_type=jnp.float32)
            part = part.reshape(lat_dev, padded, chunk)

            @pl.when(index == 0)
            def _():
                out_ref[:, :, span] = part

            @pl.when(index > 0)
            def _():
                out_ref[:, :, span] += part

            return carry

        lax.fori_loop(0, length // chunk, columns, 0)
        return carry

    lax.fori_loop(0, groups, synthesis, 0)

    def sent(index, carry):
        pltpu.make_async_copy(recv.at[index, pl.ds(0, devices - 1)], recv.at[index, pl.ds(0, devices - 1)], send_sem.at[index]).wait()
        return carry

    lax.fori_loop(0, groups, sent, 0)


def exchange(first, both, legendre, phase, lat_order, members, group, length):
    devices, rows, wide = first.shape
    slots, lats, width = legendre.shape
    groups = slots // group
    lat_dev = lats // devices
    padded = round_up(members, 8)
    depth = devices * rows
    anywhere = pl.BlockSpec(memory_space=pl.ANY)
    return pl.pallas_call(
        functools.partial(exchange_kernel, group, members),
        in_specs=[
            pl.BlockSpec(memory_space=pltpu.SMEM),
            anywhere,
            anywhere,
            anywhere,
            pl.BlockSpec(memory_space=pltpu.VMEM),
        ],
        out_specs=pl.BlockSpec(memory_space=pltpu.VMEM),
        out_shape=jax.ShapeDtypeStruct((lat_dev, padded, length), jnp.float32),
        scratch_shapes=[
            pltpu.VMEM((2, lats, width), jnp.float32),
            pltpu.VMEM((2, 2 * LANES, width), jnp.bfloat16),
            pltpu.VMEM((lats, rows, LANES), jnp.float32),
            pltpu.VMEM((max(groups - 1, 1), devices, rows, wide), jnp.float32),
            pltpu.VMEM((groups, devices, rows, wide), jnp.float32),
            pltpu.VMEM((wide, depth), jnp.float32),
            pltpu.VMEM((lat_dev, padded, 2 * depth), jnp.float32),
            pltpu.VMEM((3 * depth, length), jnp.bfloat16),
            pltpu.SemaphoreType.DMA((2, 2)),
            pltpu.SemaphoreType.DMA((groups,)),
            pltpu.SemaphoreType.DMA((groups,)),
            pltpu.SemaphoreType.DMA((groups,)),
        ],
        compiler_params=pltpu.CompilerParams(collective_id=0, has_side_effects=True),
        name="exchange",
    )(lat_order, first, both, legendre, phase)


def local(coeffs_old, noise, legendre, decay, amplitude, wavenumber_of_slot, lat_order):
    devices = lax.axis_size("lat") * lax.axis_size("lon")
    me = lax.axis_index("lat") * lax.axis_size("lon") + lax.axis_index("lon")
    slots, parts, scales, members, width = coeffs_old.shape
    lats = legendre.shape[1]
    length = 2 * lats
    lat_dev = lats // devices
    group = group_size(slots)
    groups = slots // group
    rows = round_up(parts * group, 8)
    wide = round_up(lat_dev * members, LANES)
    mine = lax.dynamic_slice_in_dim(wavenumber_of_slot, me * slots, slots)
    spread = jnp.pad(amplitude * jnp.sqrt(1.0 - decay * decay)[:, None], ((0, 8 - scales), (0, 0)))
    waves = wavenumber_of_slot.astype(jnp.float32).reshape(devices, groups, group).transpose(1, 0, 2)
    waves = jnp.pad(jnp.repeat(waves, parts, axis=2), ((0, 0), (0, 0), (0, rows - parts * group)))
    phase = jnp.broadcast_to(waves.reshape(-1, 1), (groups * devices * rows, LANES))
    turn = (0, 2, 3, 1, 4)
    new, both, first = update(
        coeffs_old.transpose(turn), noise.transpose(turn), legendre, spread, decay, mine, lat_order, devices, rows, wide, group
    )
    coeffs_new = new.transpose(0, 3, 1, 2, 4)
    out = exchange(first, both, legendre, phase, lat_order, members, group, length)
    return (coeffs_new, out[:, :members, :])


def solution(mesh):
    split_rows = ("lat", "lon")
    in_specs = (
        P(split_rows, None, None, None, None),
        P(split_rows, None, None, None, None),
        P(split_rows, None, None),
        P(),
        P(),
        P(),
        P(),
    )
    out_specs = (P(split_rows, None, None, None, None), P(split_rows, None, None))
    return jax.shard_map(local, mesh=mesh, in_specs=in_specs, out_specs=out_specs, check_vma=False)
```

```python
import functools

import jax
import jax.numpy as jnp
from jax import lax
from jax.experimental import pallas as pl
from jax.experimental.pallas import tpu as pltpu
from jax.sharding import PartitionSpec as P

TWO_PI = 6.283185307179586
LANES = 128
SUBLANES = 8
HALF = 64
PARTS = 2
MESH = pl.DeviceIdType.MESH


def round_up(size, unit):
    return -(-size // unit) * unit


def split(x):
    high = x.astype(jnp.bfloat16)
    return high, (x - high.astype(jnp.float32)).astype(jnp.bfloat16)


class Group:
    def __init__(self, size, lat_dev, members):
        used = PARTS * size
        self.size = size
        self.fold = SUBLANES // used if SUBLANES % used == 0 and lat_dev % (SUBLANES // used) == 0 else 1
        self.rows = round_up(self.fold * used, SUBLANES)
        self.padded = self.rows > self.fold * used
        self.lat = lat_dev // self.fold
        self.wide = round_up(self.lat * members, LANES)

    def block(self, devices):
        return (devices, self.rows, self.wide)


def plan(slots, lat_dev, members):
    if slots % 4 == 0 and slots >= 8:
        sizes = (2, 4, slots // 4 - 1, 2)
    elif slots > 4 and slots % 4:
        sizes = (slots % 4, 4, slots // 4 - 1, 4)
    else:
        sizes = (1, 1, slots - 2, 1)
    first, middle, count, last = sizes
    return Group(first, lat_dev, members), Group(middle, lat_dev, members), count, Group(last, lat_dev, members)


def position():
    lat_size, lon_size = lax.axis_size("lat"), lax.axis_size("lon")
    return lax.axis_index("lat") * lon_size + lax.axis_index("lon"), lat_size * lon_size, lon_size


def gains_kernel(waves_ref, decay_ref, amplitude_ref, gains_ref):
    slots, _, width = gains_ref.shape
    scales = amplitude_ref.shape[0]
    me = position()[0]
    row = lax.broadcasted_iota(jnp.int32, (SUBLANES, width), 0)
    column = lax.broadcasted_iota(jnp.int32, (SUBLANES, width), 1)
    table = jnp.zeros((SUBLANES, width), jnp.float32)
    for scale in range(scales):
        decay = jnp.full((1, width), decay_ref[scale], jnp.float32)
        table = jnp.where(row == scale, amplitude_ref[scale : scale + 1, :] * jnp.sqrt(1.0 - decay * decay), table)
        table = jnp.where(row == scales + scale, decay, table)

    def one(slot, carry):
        wave = waves_ref[me * slots + slot]
        gains_ref[slot] = jnp.where(column + wave < width, pltpu.roll(table, width - wave, axis=1), 0.0)
        return carry

    lax.fori_loop(0, slots, one, 0)


def gains_of_slots(waves, decay, amplitude, slots):
    smem = pl.BlockSpec(memory_space=pltpu.SMEM)
    vmem = pl.BlockSpec(memory_space=pltpu.VMEM)
    return pl.pallas_call(
        gains_kernel,
        in_specs=[smem, smem, vmem],
        out_specs=vmem,
        out_shape=jax.ShapeDtypeStruct((slots, SUBLANES, amplitude.shape[1]), jnp.float32),
        name="gains",
    )(waves, decay, amplitude)


def turn_block(block_ref, group, turned, left, lat_dev, members):
    devices, rows, wide = block_ref.shape
    depth = devices * rows
    turned[:wide, :depth] = block_ref[...].reshape(depth, wide).T
    column = lax.broadcasted_iota(jnp.int32, (1, depth), 1)
    fold = lax.rem(column // (PARTS * group.size), group.fold)
    for q in range(lat_dev):
        start = members * (q % group.lat)
        piece = turned[start : start + members, :depth]
        if group.fold > 1:
            piece = jnp.where(fold == q // group.lat, piece, 0.0)
        high, low = split(piece)
        left[q, :members, :depth] = high.astype(jnp.float32)
        left[q, :members, depth : 2 * depth] = low.astype(jnp.float32)


def contract(values, table, depth):
    both = jnp.dot(values, table[: 2 * depth], preferred_element_type=jnp.float32)
    return both + jnp.dot(values[:, :depth], table[2 * depth :], preferred_element_type=jnp.float32)


def exchange_kernel(
    first, middle, count, last, members,
    order_ref, waves_ref, gains_ref, old_hbm, noise_hbm, basis_hbm,
    sum_hbm, arrived_hbm, table_hbm,
    old, noise, basis, weights, field, send_first, send_middle, send_last, recv_first, recv_middle,
    wave, turned, left, table, total, load_sem, own_sem, send_sem, recv_sem, out_sem,
):
    me, devices, lon_size = position()
    slots, lats, width = basis_hbm.shape
    scales = old_hbm.shape[1]
    lat_dev, padded, length = total.shape
    final = count + 1

    def peer(other):
        return other // lon_size, lax.rem(other, lon_size)

    barrier = pltpu.get_barrier_semaphore()

    def greet(k, carry):
        pl.semaphore_signal(barrier, inc=1, device_id=peer(lax.rem(me + k, devices)), device_id_type=MESH)
        return carry

    lax.fori_loop(1, devices, greet, 0)

    def loads(slot):
        side = lax.rem(slot, 2)
        return (
            pltpu.make_async_copy(old_hbm.at[slot], old.at[side], load_sem.at[0, side]),
            pltpu.make_async_copy(noise_hbm.at[slot], noise.at[side], load_sem.at[1, side]),
            pltpu.make_async_copy(basis_hbm.at[slot], basis.at[side], load_sem.at[2, side]),
        )

    for copy in loads(0):
        copy.start()
    weights[...] = jnp.zeros_like(weights)
    if first.padded or middle.padded or last.padded:
        field[...] = jnp.zeros_like(field)

    def transform(group, start):
        for inner in range(group.size):
            slot = start + inner

            @pl.when(slot + 1 < slots)
            def _():
                for copy in loads(slot + 1):
                    copy.start()

            for copy in loads(slot):
                copy.wait()
            side = lax.rem(slot, 2)
            summed = None
            for scale in range(scales):
                fresh = gains_ref[slot, scale : scale + 1, :].reshape(1, 1, width)
                keep = gains_ref[slot, scales + scale : scales + scale + 1, :].reshape(1, 1, width)
                value = keep * old[side, scale] + fresh * noise[side, scale].astype(jnp.float32)
                summed = value if summed is None else summed + value
            for part in range(PARTS):
                weights[part * HALF : part * HALF + members, :] = summed[:, part, :]
            high, low = split(weights[...])
            basis_high, basis_low = split(basis[side])
            lanes = (((1,), (1,)), ((), ()))
            pair = lax.dot_general(basis_high, jnp.concatenate([high, low], axis=0), lanes, preferred_element_type=jnp.float32)
            small = lax.dot_general(basis_low, high, lanes, preferred_element_type=jnp.float32)
            product = pair[:, :LANES] + pair[:, LANES:] + small
            other = pltpu.roll(product, HALF, axis=1)
            for fold in range(group.fold):
                row = PARTS * (fold * group.size + inner)
                field[:, row, :] = product
                field[:, row + 1, :] = other

    def pack_and_send(group, send, recv, index):
        rows = group.rows
        lane = lax.broadcasted_iota(jnp.int32, (rows, LANES), 1)
        fold = lax.broadcasted_iota(jnp.int32, (rows, LANES), 0) // (PARTS * group.size)

        def remote(other):
            return pltpu.make_async_remote_copy(
                src_ref=send.at[other],
                dst_ref=recv.at[me],
                send_sem=send_sem.at[index],
                recv_sem=recv_sem.at[index],
                device_id=peer(other),
                device_id_type=MESH,
            )

        def one(k, carry):
            other = lax.rem(me + k, devices)
            tiles = [jnp.zeros((rows, LANES), jnp.float32) for _ in range(group.wide // LANES)]
            for q in range(lat_dev):
                piece = field[order_ref[other * lat_dev + q]][:rows]
                start = members * (q % group.lat)
                offset = start % LANES
                if offset:
                    piece = pltpu.roll(piece, offset, axis=1)
                tile = start // LANES
                keep = (lane >= offset) & (lane < offset + members)
                spill = lane < offset + members - LANES
                if group.fold > 1:
                    keep &= fold == q // group.lat
                    spill &= fold == q // group.lat
                tiles[tile] = jnp.where(keep, piece, tiles[tile])
                if offset + members > LANES:
                    tiles[tile + 1] = jnp.where(spill, piece, tiles[tile + 1])
            for position_, value in enumerate(tiles):
                send[other, :, position_ * LANES : (position_ + 1) * LANES] = value

            @pl.when(k == 1)
            def _():
                pltpu.make_async_copy(send.at[me], recv.at[me], own_sem.at[index]).start()

            @pl.when(k > 1)
            def _():
                remote(lax.rem(me + k - 1, devices)).start()

            return carry

        lax.fori_loop(0, devices, one, 0)
        remote(lax.rem(me + devices - 1, devices)).start()

    def await_group(recv, index):
        others = recv.at[pl.ds(0, devices - 1)]
        pltpu.make_async_copy(others, others, recv_sem.at[index]).wait()
        pltpu.make_async_copy(recv.at[0], recv.at[0], own_sem.at[index]).wait()

    transform(first, 0)
    pl.semaphore_wait(barrier, devices - 1)
    pack_and_send(first, send_first, recv_first, 0)

    def middle_step(step, carry):
        transform(middle, first.size + step * middle.size)
        pack_and_send(middle, send_middle.at[step], recv_middle.at[step], step + 1)
        return carry

    lax.fori_loop(0, count, middle_step, 0)
    transform(last, slots - last.size)
    pack_and_send(last, send_last, arrived_hbm, final)

    def make_table(group, start):
        rows = group.rows
        depth = devices * rows
        slot = lax.rem(lax.broadcasted_iota(jnp.int32, (rows, LANES), 0) // PARTS, group.size)

        def fill(device, carry):
            tile = jnp.zeros((rows, LANES), jnp.int32)
            for inner in range(group.size):
                tile = jnp.where(slot == inner, waves_ref[device * slots + start + inner], tile)
            wave[pl.ds(pl.multiple_of(device * rows, SUBLANES), rows), :] = tile.astype(jnp.float32)
            return carry

        lax.fori_loop(0, devices, fill, 0)
        waves = wave[:depth, :]
        lane = lax.broadcasted_iota(jnp.int32, (depth, LANES), 1).astype(jnp.float32)
        row = lax.broadcasted_iota(jnp.int32, (depth, LANES), 0)

        def angle(steps):
            turns = jnp.floor(steps * (1.0 / length))
            return (steps - turns * length) * (TWO_PI / length)

        base = angle(waves * lane) + jnp.where(lax.rem(row, PARTS) == 0, 0.0, TWO_PI / 4)
        weight = jnp.where(waves == 0.0, 1.0, 2.0)
        cosine, sine = weight * jnp.cos(base), weight * jnp.sin(base)
        stride = angle(waves * float(LANES))
        step_cosine, step_sine = jnp.cos(stride), jnp.sin(stride)
        for block in range(length // LANES):
            if block:
                cosine, sine = cosine * step_cosine - sine * step_sine, sine * step_cosine + cosine * step_sine
            high, low = split(cosine)
            span = slice(block * LANES, (block + 1) * LANES)
            table[:depth, span] = high
            table[depth : 2 * depth, span] = high
            table[2 * depth : 3 * depth, span] = low

    def synthesis(group, recv, index, start, fresh):
        depth = devices * group.rows
        make_table(group, start)
        await_group(recv, index)
        turn_block(recv, group, turned, left, lat_dev, members)
        values = left[:, :, : 2 * depth].reshape(lat_dev * padded, 2 * depth).astype(jnp.bfloat16)
        chunk = 2 * LANES

        def columns(n, carry):
            span = pl.ds(pl.multiple_of(n * chunk, chunk), chunk)
            part = contract(values, table[: 3 * depth, span], depth).reshape(lat_dev, padded, chunk)
            total[:, :, span] = part if fresh else total[:, :, span] + part
            return carry

        lax.fori_loop(0, length // chunk, columns, 0)

    left[...] = jnp.zeros_like(left)
    synthesis(first, recv_first, 0, 0, True)

    def middle_synthesis(step, carry):
        synthesis(middle, recv_middle.at[step], step + 1, first.size + step * middle.size, False)
        return carry

    lax.fori_loop(0, count, middle_synthesis, 0)
    sum_out = pltpu.make_async_copy(total, sum_hbm, out_sem.at[0])
    sum_out.start()
    make_table(last, slots - last.size)
    table_out = pltpu.make_async_copy(table.at[: table_hbm.shape[0]], table_hbm, out_sem.at[1])
    table_out.start()

    def sent(block, index):
        others = block.at[pl.ds(0, devices - 1)]
        pltpu.make_async_copy(others, others, send_sem.at[index]).wait()

    sent(send_first, 0)

    def middle_sent(step, carry):
        sent(send_middle.at[step], step + 1)
        return carry

    lax.fori_loop(0, count, middle_sent, 0)
    sum_out.wait()
    table_out.wait()
    sent(send_last, final)
    await_group(arrived_hbm, final)


def exchange(gains, old, noise, legendre, waves, lat_order, length):
    devices = lax.axis_size("lat") * lax.axis_size("lon")
    slots, scales, members, parts, width = old.shape
    lats = legendre.shape[1]
    lat_dev = lats // devices
    first, middle, count, last = plan(slots, lat_dev, members)
    groups = (first, middle, last)
    padded = round_up(members, SUBLANES)
    depth = devices * max(group.rows for group in groups)
    rows = max(group.rows for group in groups)
    some = max(count, 1)
    smem = pl.BlockSpec(memory_space=pltpu.SMEM)
    anywhere = pl.BlockSpec(memory_space=pl.ANY)
    return pl.pallas_call(
        functools.partial(exchange_kernel, first, middle, count, last, members),
        in_specs=[smem, smem, pl.BlockSpec(memory_space=pltpu.VMEM), anywhere, anywhere, anywhere],
        out_specs=[anywhere, anywhere, anywhere],
        out_shape=[
            jax.ShapeDtypeStruct((lat_dev, padded, length), jnp.float32),
            jax.ShapeDtypeStruct(last.block(devices), jnp.float32),
            jax.ShapeDtypeStruct((3 * devices * last.rows, length), jnp.bfloat16),
        ],
        scratch_shapes=[
            pltpu.VMEM((2, scales, members, parts, width), jnp.float32),
            pltpu.VMEM((2, scales, members, parts, width), jnp.bfloat16),
            pltpu.VMEM((2, lats, width), jnp.float32),
            pltpu.VMEM((LANES, width), jnp.float32),
            pltpu.VMEM((lats, rows, LANES), jnp.float32),
            pltpu.VMEM(first.block(devices), jnp.float32),
            pltpu.VMEM((some,) + middle.block(devices), jnp.float32),
            pltpu.VMEM(last.block(devices), jnp.float32),
            pltpu.VMEM(first.block(devices), jnp.float32),
            pltpu.VMEM((some,) + middle.block(devices), jnp.float32),
            pltpu.VMEM((depth, LANES), jnp.float32),
            pltpu.VMEM((max(group.wide for group in groups), depth), jnp.float32),
            pltpu.VMEM((lat_dev, padded, 2 * depth), jnp.float32),
            pltpu.VMEM((3 * depth, length), jnp.bfloat16),
            pltpu.VMEM((lat_dev, padded, length), jnp.float32),
            pltpu.SemaphoreType.DMA((3, 2)),
            pltpu.SemaphoreType.DMA((count + 2,)),
            pltpu.SemaphoreType.DMA((count + 2,)),
            pltpu.SemaphoreType.DMA((count + 2,)),
            pltpu.SemaphoreType.DMA((2,)),
        ],
        compiler_params=pltpu.CompilerParams(collective_id=0, has_side_effects=True),
        name="exchange",
    )(lat_order, waves, gains, old, noise, legendre)


def finish_kernel(group, members, sum_ref, arrived_ref, table_ref, out_ref, turned, left):
    lat_dev, padded, chunk = sum_ref.shape
    depth = left.shape[2] // 2

    @pl.when(pl.program_id(0) == 0)
    def _():
        left[...] = jnp.zeros_like(left)
        turn_block(arrived_ref, group, turned, left, lat_dev, members)

    values = left[...].reshape(lat_dev * padded, 2 * depth).astype(jnp.bfloat16)
    part = sum_ref[...] + contract(values, table_ref[...], depth).reshape(lat_dev, padded, chunk)
    out_ref[...] = part[:, :members, :]


def finish(summed, arrived, table, slots, members):
    lat_dev, padded, length = summed.shape
    group = plan(slots, lat_dev, members)[3]
    devices, rows, wide = arrived.shape
    depth = devices * rows
    chunk = 2 * LANES
    return pl.pallas_call(
        functools.partial(finish_kernel, group, members),
        grid=(length // chunk,),
        in_specs=[
            pl.BlockSpec((lat_dev, padded, chunk), lambda n: (0, 0, n)),
            pl.BlockSpec((devices, rows, wide), lambda n: (0, 0, 0)),
            pl.BlockSpec((3 * depth, chunk), lambda n: (0, n)),
        ],
        out_specs=pl.BlockSpec((lat_dev, members, chunk), lambda n: (0, 0, n)),
        out_shape=jax.ShapeDtypeStruct((lat_dev, members, length), jnp.float32),
        scratch_shapes=[
            pltpu.VMEM((wide, depth), jnp.float32),
            pltpu.VMEM((lat_dev, padded, 2 * depth), jnp.float32),
        ],
        compiler_params=pltpu.CompilerParams(dimension_semantics=("arbitrary",)),
        name="finish",
    )(summed, arrived, table)


def local(coeffs_old, noise, legendre, decay, amplitude, wavenumber_of_slot, lat_order):
    slots, parts, scales, members, width = coeffs_old.shape
    length = 2 * legendre.shape[1]
    gains = gains_of_slots(wavenumber_of_slot, decay, amplitude, slots)
    fresh = gains[:, None, :scales, None, :]
    keep = gains[:, None, scales : 2 * scales, None, :]
    coeffs_new = keep * coeffs_old + fresh * noise.astype(jnp.float32)
    turn = (0, 2, 3, 1, 4)
    summed, arrived, table = exchange(
        gains, coeffs_old.transpose(turn), noise.transpose(turn), legendre, wavenumber_of_slot, lat_order, length
    )
    pattern = finish(summed, arrived, table, slots, members)
    return (coeffs_new, pattern)


def solution(mesh):
    split_rows = ("lat", "lon")
    in_specs = (
        P(split_rows, None, None, None, None),
        P(split_rows, None, None, None, None),
        P(split_rows, None, None),
        P(),
        P(),
        P(),
        P(),
    )
    out_specs = (P(split_rows, None, None, None, None), P(split_rows, None, None))
    return jax.shard_map(local, mesh=mesh, in_specs=in_specs, out_specs=out_specs, check_vma=False)
```

```python
import functools

import jax
import jax.numpy as jnp
from jax import lax
from jax.experimental import pallas as pl
from jax.experimental.pallas import tpu as pltpu
from jax.sharding import PartitionSpec as P

TWO_PI = 6.283185307179586
LANES = 128
SUBLANES = 8
HALF = 64
PARTS = 2
VMEM_LIMIT = 40 << 20
FINISH_LIMIT = 20 << 20
MESH = pl.DeviceIdType.MESH


def round_up(size, unit):
    return -(-size // unit) * unit


def split(x):
    high = x.astype(jnp.bfloat16)
    return high, (x - high.astype(jnp.float32)).astype(jnp.bfloat16)


class Group:
    def __init__(self, size, lat_dev, members):
        used = PARTS * size
        self.size = size
        self.fold = SUBLANES // used if SUBLANES % used == 0 and lat_dev % (SUBLANES // used) == 0 else 1
        self.rows = round_up(self.fold * used, SUBLANES)
        self.padded = self.rows > self.fold * used
        self.lat = lat_dev // self.fold
        self.wide = round_up(self.lat * members, LANES)

    def block(self, devices):
        return (devices, self.rows, self.wide)


def plan(slots, lat_dev, members):
    if slots % 4 == 0 and slots >= 8:
        sizes = (2, 4, slots // 4 - 1, 2)
    elif slots > 4 and slots % 4:
        sizes = (slots % 4, 4, slots // 4 - 1, 4)
    else:
        sizes = (1, 1, slots - 2, 1)
    first, middle, count, last = sizes
    return Group(first, lat_dev, members), Group(middle, lat_dev, members), count, Group(last, lat_dev, members)


def position():
    lat_size, lon_size = lax.axis_size("lat"), lax.axis_size("lon")
    return lax.axis_index("lat") * lon_size + lax.axis_index("lon"), lat_size * lon_size, lon_size


def turn_block(block_ref, group, turned, left, lat_dev, members):
    devices, rows, wide = block_ref.shape
    depth = devices * rows
    turned[:wide, :depth] = block_ref[...].reshape(depth, wide).T
    column = lax.broadcasted_iota(jnp.int32, (1, depth), 1)
    fold = lax.rem(column // (PARTS * group.size), group.fold)
    for q in range(lat_dev):
        start = members * (q % group.lat)
        piece = turned[start : start + members, :depth]
        if group.fold > 1:
            piece = jnp.where(fold == q // group.lat, piece, 0.0)
        high, low = split(piece)
        left[q, :members, :depth] = high.astype(jnp.float32)
        left[q, :members, depth : 2 * depth] = low.astype(jnp.float32)


def contract(values, table, depth):
    both = jnp.dot(values, table[: 2 * depth], preferred_element_type=jnp.float32)
    return both + jnp.dot(values[:, :depth], table[2 * depth :], preferred_element_type=jnp.float32)


def exchange_kernel(
    first, middle, count, last, members,
    order_ref, waves_ref, decay_ref, amplitude_ref, old_hbm, noise_hbm, basis_hbm,
    new_hbm, sum_hbm, arrived_hbm, table_hbm,
    old, noise, basis, new, base_gains, gains, weights, field, send_first, send_middle, send_last, recv_first, recv_middle,
    wave, turned, left, table, total, load_sem, new_sem, own_sem, send_sem, recv_sem, out_sem,
):
    me, devices, lon_size = position()
    slots, lats, width = basis_hbm.shape
    scales = old_hbm.shape[1]
    lat_dev, padded, length = total.shape
    final = count + 1

    def peer(other):
        return other // lon_size, lax.rem(other, lon_size)

    barrier = pltpu.get_barrier_semaphore()

    def greet(k, carry):
        pl.semaphore_signal(barrier, inc=1, device_id=peer(lax.rem(me + k, devices)), device_id_type=MESH)
        return carry

    lax.fori_loop(1, devices, greet, 0)

    def loads(slot):
        side = lax.rem(slot, 2)
        return (
            pltpu.make_async_copy(old_hbm.at[slot], old.at[side], load_sem.at[0, side]),
            pltpu.make_async_copy(noise_hbm.at[slot], noise.at[side], load_sem.at[1, side]),
            pltpu.make_async_copy(basis_hbm.at[slot], basis.at[side], load_sem.at[2, side]),
        )

    for copy in loads(0):
        copy.start()
    weights[...] = jnp.zeros_like(weights)
    base_gains[...] = jnp.zeros_like(base_gains)
    for scale in range(scales):
        decay = jnp.full((1, width), decay_ref[scale], jnp.float32)
        base_gains[scale : scale + 1, :] = amplitude_ref[scale : scale + 1, :] * jnp.sqrt(1.0 - decay * decay)
        base_gains[scales + scale : scales + scale + 1, :] = decay
    column = lax.broadcasted_iota(jnp.int32, (SUBLANES, width), 1)

    def store_new(slot):
        side = lax.rem(slot, 2)
        return pltpu.make_async_copy(new.at[side], new_hbm.at[slot], new_sem.at[side])

    if first.padded or middle.padded or last.padded:
        field[...] = jnp.zeros_like(field)

    def transform(group, start):
        for inner in range(group.size):
            slot = start + inner

            @pl.when(slot + 1 < slots)
            def _():
                for copy in loads(slot + 1):
                    copy.start()

            for copy in loads(slot):
                copy.wait()
            side = lax.rem(slot, 2)
            wave_here = waves_ref[me * slots + slot]
            gains[...] = jnp.where(column + wave_here < width, pltpu.roll(base_gains[...], width - wave_here, axis=1), 0.0)

            @pl.when(slot > 1)
            def _():
                store_new(slot - 2).wait()

            summed = None
            for scale in range(scales):
                fresh = gains[scale : scale + 1, :].reshape(1, 1, width)
                keep = gains[scales + scale : scales + scale + 1, :].reshape(1, 1, width)
                value = keep * old[side, scale] + fresh * noise[side, scale].astype(jnp.float32)
                new[side, scale] = value
                summed = value if summed is None else summed + value
            store_new(slot).start()
            for part in range(PARTS):
                weights[part * HALF : part * HALF + members, :] = summed[:, part, :]
            high, low = split(weights[...])
            basis_high, basis_low = split(basis[side])
            lanes = (((1,), (1,)), ((), ()))
            pair = lax.dot_general(basis_high, jnp.concatenate([high, low], axis=0), lanes, preferred_element_type=jnp.float32)
            small = lax.dot_general(basis_low, high, lanes, preferred_element_type=jnp.float32)
            product = pair[:, :LANES] + pair[:, LANES:] + small
            other = pltpu.roll(product, HALF, axis=1)
            for fold in range(group.fold):
                row = PARTS * (fold * group.size + inner)
                field[:, row, :] = product
                field[:, row + 1, :] = other

    def pack_and_send(group, send, recv, index):
        rows = group.rows
        lane = lax.broadcasted_iota(jnp.int32, (rows, LANES), 1)
        fold = lax.broadcasted_iota(jnp.int32, (rows, LANES), 0) // (PARTS * group.size)

        def remote(other):
            return pltpu.make_async_remote_copy(
                src_ref=send.at[other],
                dst_ref=recv.at[me],
                send_sem=send_sem.at[index],
                recv_sem=recv_sem.at[index],
                device_id=peer(other),
                device_id_type=MESH,
            )

        def one(k, carry):
            other = lax.rem(me + k, devices)
            tiles = [jnp.zeros((rows, LANES), jnp.float32) for _ in range(group.wide // LANES)]
            for q in range(lat_dev):
                piece = field[order_ref[other * lat_dev + q]][:rows]
                start = members * (q % group.lat)
                offset = start % LANES
                if offset:
                    piece = pltpu.roll(piece, offset, axis=1)
                tile = start // LANES
                keep = (lane >= offset) & (lane < offset + members)
                spill = lane < offset + members - LANES
                if group.fold > 1:
                    keep &= fold == q // group.lat
                    spill &= fold == q // group.lat
                tiles[tile] = jnp.where(keep, piece, tiles[tile])
                if offset + members > LANES:
                    tiles[tile + 1] = jnp.where(spill, piece, tiles[tile + 1])
            for position_, value in enumerate(tiles):
                send[other, :, position_ * LANES : (position_ + 1) * LANES] = value

            @pl.when(k == 1)
            def _():
                pltpu.make_async_copy(send.at[me], recv.at[me], own_sem.at[index]).start()

            @pl.when(k > 1)
            def _():
                remote(lax.rem(me + k - 1, devices)).start()

            return carry

        lax.fori_loop(0, devices, one, 0)
        remote(lax.rem(me + devices - 1, devices)).start()

    def await_group(recv, index):
        others = recv.at[pl.ds(0, devices - 1)]
        pltpu.make_async_copy(others, others, recv_sem.at[index]).wait()
        pltpu.make_async_copy(recv.at[0], recv.at[0], own_sem.at[index]).wait()

    transform(first, 0)
    pl.semaphore_wait(barrier, devices - 1)
    pack_and_send(first, send_first, recv_first, 0)

    def middle_step(step, carry):
        transform(middle, first.size + step * middle.size)
        pack_and_send(middle, send_middle.at[step], recv_middle.at[step], step + 1)
        return carry

    lax.fori_loop(0, count, middle_step, 0)
    transform(last, slots - last.size)
    pack_and_send(last, send_last, arrived_hbm, final)
    for slot in range(max(slots - 2, 0), slots):
        store_new(slot).wait()

    def make_table(group, start):
        rows = group.rows
        depth = devices * rows
        slot = lax.rem(lax.broadcasted_iota(jnp.int32, (rows, LANES), 0) // PARTS, group.size)

        def fill(device, carry):
            tile = jnp.zeros((rows, LANES), jnp.int32)
            for inner in range(group.size):
                tile = jnp.where(slot == inner, waves_ref[device * slots + start + inner], tile)
            wave[pl.ds(pl.multiple_of(device * rows, SUBLANES), rows), :] = tile.astype(jnp.float32)
            return carry

        lax.fori_loop(0, devices, fill, 0)
        waves = wave[:depth, :]
        lane = lax.broadcasted_iota(jnp.int32, (depth, LANES), 1).astype(jnp.float32)
        row = lax.broadcasted_iota(jnp.int32, (depth, LANES), 0)

        def angle(steps):
            turns = jnp.floor(steps * (1.0 / length))
            return (steps - turns * length) * (TWO_PI / length)

        base = angle(waves * lane) + jnp.where(lax.rem(row, PARTS) == 0, 0.0, TWO_PI / 4)
        weight = jnp.where(waves == 0.0, 1.0, 2.0)
        cosine, sine = weight * jnp.cos(base), weight * jnp.sin(base)
        stride = angle(waves * float(LANES))
        step_cosine, step_sine = jnp.cos(stride), jnp.sin(stride)
        for block in range(length // LANES):
            if block:
                cosine, sine = cosine * step_cosine - sine * step_sine, sine * step_cosine + cosine * step_sine
            high, low = split(cosine)
            span = slice(block * LANES, (block + 1) * LANES)
            table[:depth, span] = high
            table[depth : 2 * depth, span] = high
            table[2 * depth : 3 * depth, span] = low

    def synthesis(group, recv, index, start, fresh):
        depth = devices * group.rows
        make_table(group, start)
        await_group(recv, index)
        turn_block(recv, group, turned, left, lat_dev, members)
        values = left[:, :, : 2 * depth].reshape(lat_dev * padded, 2 * depth).astype(jnp.bfloat16)
        chunk = 2 * LANES

        def columns(n, carry):
            span = pl.ds(pl.multiple_of(n * chunk, chunk), chunk)
            part = contract(values, table[: 3 * depth, span], depth).reshape(lat_dev, padded, chunk)
            total[:, :, span] = part if fresh else total[:, :, span] + part
            return carry

        lax.fori_loop(0, length // chunk, columns, 0)

    left[...] = jnp.zeros_like(left)
    synthesis(first, recv_first, 0, 0, True)

    def middle_synthesis(step, carry):
        synthesis(middle, recv_middle.at[step], step + 1, first.size + step * middle.size, False)
        return carry

    lax.fori_loop(0, count, middle_synthesis, 0)
    sum_out = pltpu.make_async_copy(total, sum_hbm, out_sem.at[0])
    sum_out.start()
    make_table(last, slots - last.size)
    table_out = pltpu.make_async_copy(table.at[: table_hbm.shape[0]], table_hbm, out_sem.at[1])
    table_out.start()

    def sent(block, index):
        others = block.at[pl.ds(0, devices - 1)]
        pltpu.make_async_copy(others, others, send_sem.at[index]).wait()

    sent(send_first, 0)

    def middle_sent(step, carry):
        sent(send_middle.at[step], step + 1)
        return carry

    lax.fori_loop(0, count, middle_sent, 0)
    sum_out.wait()
    table_out.wait()
    sent(send_last, final)
    await_group(arrived_hbm, final)


def exchange(old, noise, legendre, decay, amplitude, waves, lat_order, length):
    devices = lax.axis_size("lat") * lax.axis_size("lon")
    slots, scales, members, parts, width = old.shape
    lats = legendre.shape[1]
    lat_dev = lats // devices
    first, middle, count, last = plan(slots, lat_dev, members)
    groups = (first, middle, last)
    padded = round_up(members, SUBLANES)
    depth = devices * max(group.rows for group in groups)
    rows = max(group.rows for group in groups)
    some = max(count, 1)
    smem = pl.BlockSpec(memory_space=pltpu.SMEM)
    anywhere = pl.BlockSpec(memory_space=pl.ANY)
    hbm = pl.BlockSpec(memory_space=pltpu.HBM)
    return pl.pallas_call(
        functools.partial(exchange_kernel, first, middle, count, last, members),
        in_specs=[smem, smem, smem, pl.BlockSpec(memory_space=pltpu.VMEM), hbm, hbm, hbm],
        out_specs=[anywhere, anywhere, anywhere, anywhere],
        out_shape=[
            jax.ShapeDtypeStruct(old.shape, jnp.float32),
            jax.ShapeDtypeStruct((lat_dev, padded, length), jnp.float32),
            jax.ShapeDtypeStruct(last.block(devices), jnp.float32),
            jax.ShapeDtypeStruct((3 * devices * last.rows, length), jnp.bfloat16),
        ],
        scratch_shapes=[
            pltpu.VMEM((2, scales, members, parts, width), jnp.float32),
            pltpu.VMEM((2, scales, members, parts, width), jnp.bfloat16),
            pltpu.VMEM((2, lats, width), jnp.float32),
            pltpu.VMEM((2, scales, members, parts, width), jnp.float32),
            pltpu.VMEM((SUBLANES, width), jnp.float32),
            pltpu.VMEM((SUBLANES, width), jnp.float32),
            pltpu.VMEM((LANES, width), jnp.float32),
            pltpu.VMEM((lats, rows, LANES), jnp.float32),
            pltpu.VMEM(first.block(devices), jnp.float32),
            pltpu.VMEM((some,) + middle.block(devices), jnp.float32),
            pltpu.VMEM(last.block(devices), jnp.float32),
            pltpu.VMEM(first.block(devices), jnp.float32),
            pltpu.VMEM((some,) + middle.block(devices), jnp.float32),
            pltpu.VMEM((depth, LANES), jnp.float32),
            pltpu.VMEM((max(group.wide for group in groups), depth), jnp.float32),
            pltpu.VMEM((lat_dev, padded, 2 * depth), jnp.float32),
            pltpu.VMEM((3 * depth, length), jnp.bfloat16),
            pltpu.VMEM((lat_dev, padded, length), jnp.float32),
            pltpu.SemaphoreType.DMA((3, 2)),
            pltpu.SemaphoreType.DMA((2,)),
            pltpu.SemaphoreType.DMA((count + 2,)),
            pltpu.SemaphoreType.DMA((count + 2,)),
            pltpu.SemaphoreType.DMA((count + 2,)),
            pltpu.SemaphoreType.DMA((2,)),
        ],
        compiler_params=pltpu.CompilerParams(collective_id=0, has_side_effects=True, vmem_limit_bytes=VMEM_LIMIT),
        name="exchange",
    )(lat_order, waves, decay, amplitude, old, noise, legendre)


def finish_kernel(group, members, sum_ref, arrived_ref, table_ref, out_ref, turned, left):
    lat_dev, padded, _ = sum_ref.shape
    chunk = out_ref.shape[2]
    depth = left.shape[2] // 2
    step = pl.program_id(0)

    @pl.when(step == 0)
    def _():
        left[...] = jnp.zeros_like(left)
        turn_block(arrived_ref, group, turned, left, lat_dev, members)

    span = pl.ds(pl.multiple_of(step * chunk, chunk), chunk)
    values = left[...].reshape(lat_dev * padded, 2 * depth).astype(jnp.bfloat16)
    part = sum_ref[:, :, span] + contract(values, table_ref[:, span], depth).reshape(lat_dev, padded, chunk)
    out_ref[...] = part[:, :members, :]


def finish(summed, arrived, table, slots, members):
    lat_dev, padded, length = summed.shape
    group = plan(slots, lat_dev, members)[3]
    devices, rows, wide = arrived.shape
    depth = devices * rows
    chunk = 2 * LANES
    vmem = pl.BlockSpec(memory_space=pltpu.VMEM)
    return pl.pallas_call(
        functools.partial(finish_kernel, group, members),
        grid=(length // chunk,),
        in_specs=[vmem, vmem, vmem],
        out_specs=pl.BlockSpec((lat_dev, members, chunk), lambda n: (0, 0, n)),
        out_shape=jax.ShapeDtypeStruct((lat_dev, members, length), jnp.float32),
        scratch_shapes=[
            pltpu.VMEM((wide, depth), jnp.float32),
            pltpu.VMEM((lat_dev, padded, 2 * depth), jnp.float32),
        ],
        compiler_params=pltpu.CompilerParams(dimension_semantics=("arbitrary",), vmem_limit_bytes=FINISH_LIMIT),
        name="finish",
    )(summed, arrived, table)


def local(coeffs_old, noise, legendre, decay, amplitude, wavenumber_of_slot, lat_order):
    slots, parts, scales, members, width = coeffs_old.shape
    length = 2 * legendre.shape[1]
    turn = (0, 2, 3, 1, 4)
    new, summed, arrived, table = exchange(
        coeffs_old.transpose(turn), noise.transpose(turn), legendre, decay, amplitude, wavenumber_of_slot, lat_order, length
    )
    coeffs_new = new.transpose(0, 3, 1, 2, 4)
    pattern = finish(summed, arrived, table, slots, members)
    return (coeffs_new, pattern)


def solution(mesh):
    split_rows = ("lat", "lon")
    in_specs = (
        P(split_rows, None, None, None, None),
        P(split_rows, None, None, None, None),
        P(split_rows, None, None),
        P(),
        P(),
        P(),
        P(),
    )
    out_specs = (P(split_rows, None, None, None, None), P(split_rows, None, None))
    return jax.shard_map(local, mesh=mesh, in_specs=in_specs, out_specs=out_specs, check_vma=False)
```

```python
import functools

import jax
import jax.numpy as jnp
from jax import lax
from jax.experimental import pallas as pl
from jax.experimental.pallas import tpu as pltpu
from jax.sharding import PartitionSpec as P

TWO_PI = 6.283185307179586
LANES = 128
SUBLANES = 8
HALF = 64
PARTS = 2
VMEM_LIMIT = 28 << 20
FINISH_LIMIT = 16 << 20
MESH = pl.DeviceIdType.MESH


def round_up(size, unit):
    return -(-size // unit) * unit


def split(x):
    high = x.astype(jnp.bfloat16)
    return high, (x - high.astype(jnp.float32)).astype(jnp.bfloat16)


class Group:
    def __init__(self, size, lat_dev, members):
        used = PARTS * size
        self.size = size
        self.fold = SUBLANES // used if SUBLANES % used == 0 and lat_dev % (SUBLANES // used) == 0 else 1
        self.rows = round_up(self.fold * used, SUBLANES)
        self.padded = self.rows > self.fold * used
        self.lat = lat_dev // self.fold
        self.wide = round_up(self.lat * members, LANES)

    def block(self, devices):
        return (devices, self.rows, self.wide)


def plan(slots, lat_dev, members):
    if slots % 4 == 0 and slots >= 8:
        sizes, size = (1, 1, 2), 4
    elif slots > 4:
        sizes, size = (slots % 4,), 4
    else:
        sizes, size = (), 1
    leaders = [Group(size_, lat_dev, members) for size_ in sizes]
    return leaders, Group(size, lat_dev, members), (slots - sum(sizes)) // size


def position():
    lat_size, lon_size = lax.axis_size("lat"), lax.axis_size("lon")
    return lax.axis_index("lat") * lon_size + lax.axis_index("lon"), lat_size * lon_size, lon_size


def turn_block(block_ref, group, turned, left, lat_dev, members):
    devices, rows, wide = block_ref.shape
    depth = devices * rows
    turned[:wide, :depth] = block_ref[...].reshape(depth, wide).T
    column = lax.broadcasted_iota(jnp.int32, (1, depth), 1)
    fold = lax.rem(column // (PARTS * group.size), group.fold)
    for q in range(lat_dev):
        start = members * (q % group.lat)
        piece = turned[start : start + members, :depth]
        if group.fold > 1:
            piece = jnp.where(fold == q // group.lat, piece, 0.0)
        high, low = split(piece)
        left[q, :members, :depth] = high.astype(jnp.float32)
        left[q, :members, depth : 2 * depth] = low.astype(jnp.float32)


def contract(values, table, depth):
    both = jnp.dot(values, table[: 2 * depth], preferred_element_type=jnp.float32)
    return both + jnp.dot(values[:, :depth], table[2 * depth :], preferred_element_type=jnp.float32)


def exchange_kernel(
    leaders, middle, count, members,
    order_ref, waves_ref, decay_ref, amplitude_ref, old_hbm, noise_hbm, basis_hbm,
    *refs,
):
    scales = old_hbm.shape[1]
    new = refs[:scales]
    (
        total, recv_middle, table,
        old, noise, basis, base_gains, gains, weights, field, send_lead, recv_lead, send_middle,
        wave, turned, left, load_sem, own_sem, send_sem, recv_sem,
    ) = refs[scales:]
    me, devices, lon_size = position()
    slots, lats, width = basis_hbm.shape
    lat_dev, padded, length = total.shape
    lead = len(leaders)
    starts = [sum(group.size for group in leaders[:index]) for index in range(lead + 1)]

    def peer(other):
        return other // lon_size, lax.rem(other, lon_size)

    barrier = pltpu.get_barrier_semaphore()

    def greet(k, carry):
        pl.semaphore_signal(barrier, inc=1, device_id=peer(lax.rem(me + k, devices)), device_id_type=MESH)
        return carry

    lax.fori_loop(1, devices, greet, 0)

    def loads(slot):
        side = lax.rem(slot, 2)
        return (
            pltpu.make_async_copy(old_hbm.at[slot], old.at[side], load_sem.at[0, side]),
            pltpu.make_async_copy(noise_hbm.at[slot], noise.at[side], load_sem.at[1, side]),
            pltpu.make_async_copy(basis_hbm.at[slot], basis.at[side], load_sem.at[2, side]),
        )

    for copy in loads(0):
        copy.start()
    weights[...] = jnp.zeros_like(weights)
    base_gains[...] = jnp.zeros_like(base_gains)
    for scale in range(scales):
        decay = jnp.full((1, width), decay_ref[scale], jnp.float32)
        base_gains[scale : scale + 1, :] = amplitude_ref[scale : scale + 1, :] * jnp.sqrt(1.0 - decay * decay)
        base_gains[scales + scale : scales + scale + 1, :] = decay
    column = lax.broadcasted_iota(jnp.int32, (SUBLANES, width), 1)

    if any(group.padded for group in leaders + [middle]):
        field[...] = jnp.zeros_like(field)

    def transform(group, start):
        for inner in range(group.size):
            slot = start + inner

            @pl.when(slot + 1 < slots)
            def _():
                for copy in loads(slot + 1):
                    copy.start()

            for copy in loads(slot):
                copy.wait()
            side = lax.rem(slot, 2)
            wave_here = waves_ref[me * slots + slot]
            gains[...] = jnp.where(column + wave_here < width, pltpu.roll(base_gains[...], width - wave_here, axis=1), 0.0)

            summed = None
            for scale in range(scales):
                fresh = gains[scale : scale + 1, :].reshape(1, 1, width)
                keep = gains[scales + scale : scales + scale + 1, :].reshape(1, 1, width)
                value = keep * old[side, scale] + fresh * noise[side, scale].astype(jnp.float32)
                new[scale][slot] = value
                summed = value if summed is None else summed + value
            for part in range(PARTS):
                weights[part * HALF : part * HALF + members, :] = summed[:, part, :]
            high, low = split(weights[...])
            basis_high, basis_low = split(basis[side])
            lanes = (((1,), (1,)), ((), ()))
            pair = lax.dot_general(basis_high, jnp.concatenate([high, low], axis=0), lanes, preferred_element_type=jnp.float32)
            small = lax.dot_general(basis_low, high, lanes, preferred_element_type=jnp.float32)
            product = pair[:, :LANES] + pair[:, LANES:] + small
            other = pltpu.roll(product, HALF, axis=1)
            for fold in range(group.fold):
                row = PARTS * (fold * group.size + inner)
                field[:, row, :] = product
                field[:, row + 1, :] = other

    def pack_and_send(group, send, recv, index):
        rows = group.rows
        lane = lax.broadcasted_iota(jnp.int32, (rows, LANES), 1)
        fold = lax.broadcasted_iota(jnp.int32, (rows, LANES), 0) // (PARTS * group.size)

        def remote(other):
            return pltpu.make_async_remote_copy(
                src_ref=send.at[other],
                dst_ref=recv.at[me],
                send_sem=send_sem.at[index],
                recv_sem=recv_sem.at[index],
                device_id=peer(other),
                device_id_type=MESH,
            )

        def one(k, carry):
            other = lax.rem(me + k, devices)
            tiles = [jnp.zeros((rows, LANES), jnp.float32) for _ in range(group.wide // LANES)]
            for q in range(lat_dev):
                piece = field[order_ref[other * lat_dev + q]][:rows]
                start = members * (q % group.lat)
                offset = start % LANES
                if offset:
                    piece = pltpu.roll(piece, offset, axis=1)
                tile = start // LANES
                keep = (lane >= offset) & (lane < offset + members)
                spill = lane < offset + members - LANES
                if group.fold > 1:
                    keep &= fold == q // group.lat
                    spill &= fold == q // group.lat
                tiles[tile] = jnp.where(keep, piece, tiles[tile])
                if offset + members > LANES:
                    tiles[tile + 1] = jnp.where(spill, piece, tiles[tile + 1])
            for position_, value in enumerate(tiles):
                send[other, :, position_ * LANES : (position_ + 1) * LANES] = value

            @pl.when(k == 1)
            def _():
                pltpu.make_async_copy(send.at[me], recv.at[me], own_sem.at[index]).start()

            @pl.when(k > 1)
            def _():
                remote(lax.rem(me + k - 1, devices)).start()

            return carry

        lax.fori_loop(0, devices, one, 0)
        remote(lax.rem(me + devices - 1, devices)).start()

    def await_group(recv, index):
        others = recv.at[pl.ds(0, devices - 1)]
        pltpu.make_async_copy(others, others, recv_sem.at[index]).wait()
        pltpu.make_async_copy(recv.at[0], recv.at[0], own_sem.at[index]).wait()

    for index, group in enumerate(leaders):
        transform(group, starts[index])
        if index == 0:
            pl.semaphore_wait(barrier, devices - 1)
        pack_and_send(group, send_lead[index], recv_lead[index], index)
    if not leaders:
        pl.semaphore_wait(barrier, devices - 1)

    def middle_step(step, carry):
        transform(middle, starts[lead] + step * middle.size)
        pack_and_send(middle, send_middle.at[step], recv_middle.at[step], step + lead)
        return carry

    lax.fori_loop(0, count, middle_step, 0)

    def make_table(group, start):
        rows = group.rows
        depth = devices * rows
        slot = lax.rem(lax.broadcasted_iota(jnp.int32, (rows, LANES), 0) // PARTS, group.size)

        def fill(device, carry):
            tile = jnp.zeros((rows, LANES), jnp.int32)
            for inner in range(group.size):
                tile = jnp.where(slot == inner, waves_ref[device * slots + start + inner], tile)
            wave[pl.ds(pl.multiple_of(device * rows, SUBLANES), rows), :] = tile.astype(jnp.float32)
            return carry

        lax.fori_loop(0, devices, fill, 0)
        waves = wave[:depth, :]
        lane = lax.broadcasted_iota(jnp.int32, (depth, LANES), 1).astype(jnp.float32)
        row = lax.broadcasted_iota(jnp.int32, (depth, LANES), 0)

        def angle(steps):
            turns = jnp.floor(steps * (1.0 / length))
            return (steps - turns * length) * (TWO_PI / length)

        base = angle(waves * lane) + jnp.where(lax.rem(row, PARTS) == 0, 0.0, TWO_PI / 4)
        weight = jnp.where(waves == 0.0, 1.0, 2.0)
        cosine, sine = weight * jnp.cos(base), weight * jnp.sin(base)
        stride = angle(waves * float(LANES))
        step_cosine, step_sine = jnp.cos(stride), jnp.sin(stride)
        for block in range(length // LANES):
            if block:
                cosine, sine = cosine * step_cosine - sine * step_sine, sine * step_cosine + cosine * step_sine
            high, low = split(cosine)
            span = slice(block * LANES, (block + 1) * LANES)
            table[:depth, span] = high
            table[depth : 2 * depth, span] = high
            table[2 * depth : 3 * depth, span] = low

    def synthesis(group, recv, index):
        depth = devices * group.rows
        await_group(recv, index)
        turn_block(recv, group, turned, left, lat_dev, members)
        values = left[:, :, : 2 * depth].reshape(lat_dev * padded, 2 * depth).astype(jnp.bfloat16)
        chunk = 2 * LANES

        def columns(n, carry):
            span = pl.ds(pl.multiple_of(n * chunk, chunk), chunk)
            total[:, :, span] += contract(values, table[: 3 * depth, span], depth).reshape(lat_dev, padded, chunk)
            return carry

        lax.fori_loop(0, length // chunk, columns, 0)

    left[...] = jnp.zeros_like(left)
    total[...] = jnp.zeros_like(total)
    for index, group in enumerate(leaders):
        make_table(group, starts[index])
        synthesis(group, recv_lead[index], index)

    def middle_synthesis(step, carry):
        make_table(middle, starts[lead] + step * middle.size)

        @pl.when(step < count - 1)
        def _():
            synthesis(middle, recv_middle.at[step], step + lead)

        return carry

    lax.fori_loop(0, count, middle_synthesis, 0)

    def sent(block, index):
        others = block.at[pl.ds(0, devices - 1)]
        pltpu.make_async_copy(others, others, send_sem.at[index]).wait()

    for index in range(lead):
        sent(send_lead[index], index)

    def middle_sent(step, carry):
        sent(send_middle.at[step], step + lead)
        return carry

    lax.fori_loop(0, count, middle_sent, 0)
    await_group(recv_middle.at[count - 1], lead + count - 1)


def exchange(old, noise, legendre, decay, amplitude, waves, lat_order, length):
    devices = lax.axis_size("lat") * lax.axis_size("lon")
    slots, scales, members, parts, width = old.shape
    lats = legendre.shape[1]
    lat_dev = lats // devices
    leaders, middle, count = plan(slots, lat_dev, members)
    groups = leaders + [middle]
    lead_blocks = tuple(pltpu.VMEM(group.block(devices), jnp.float32) for group in leaders)
    padded = round_up(members, SUBLANES)
    rows = max(group.rows for group in groups)
    depth = devices * rows
    smem = pl.BlockSpec(memory_space=pltpu.SMEM)
    vmem = pl.BlockSpec(memory_space=pltpu.VMEM)
    hbm = pl.BlockSpec(memory_space=pltpu.HBM)
    large = [pltpu.with_memory_space_constraint(array, pltpu.HBM) for array in (old, noise, legendre)]
    return pl.pallas_call(
        functools.partial(exchange_kernel, leaders, middle, count, members),
        in_specs=[smem, smem, smem, vmem, hbm, hbm, hbm],
        out_specs=[vmem] * (scales + 3),
        out_shape=[pltpu.VMEM((slots, members, parts, width), jnp.float32)] * scales
        + [
            pltpu.VMEM((lat_dev, padded, length), jnp.float32),
            pltpu.VMEM((count,) + middle.block(devices), jnp.float32),
            pltpu.VMEM((3 * depth, length), jnp.bfloat16),
        ],
        scratch_shapes=[
            pltpu.VMEM((2, scales, members, parts, width), jnp.float32),
            pltpu.VMEM((2, scales, members, parts, width), jnp.bfloat16),
            pltpu.VMEM((2, lats, width), jnp.float32),
            pltpu.VMEM((SUBLANES, width), jnp.float32),
            pltpu.VMEM((SUBLANES, width), jnp.float32),
            pltpu.VMEM((LANES, width), jnp.float32),
            pltpu.VMEM((lats, rows, LANES), jnp.float32),
            lead_blocks,
            lead_blocks,
            pltpu.VMEM((count,) + middle.block(devices), jnp.float32),
            pltpu.VMEM((depth, LANES), jnp.float32),
            pltpu.VMEM((max(group.wide for group in groups), depth), jnp.float32),
            pltpu.VMEM((lat_dev, padded, 2 * depth), jnp.float32),
            pltpu.SemaphoreType.DMA((3, 2)),
            pltpu.SemaphoreType.DMA((len(leaders) + count,)),
            pltpu.SemaphoreType.DMA((len(leaders) + count,)),
            pltpu.SemaphoreType.DMA((len(leaders) + count,)),
        ],
        compiler_params=pltpu.CompilerParams(collective_id=0, has_side_effects=True, vmem_limit_bytes=VMEM_LIMIT),
        name="exchange",
    )(lat_order, waves, decay, amplitude, *large)


def finish_kernel(group, members, scales, *refs):
    new = refs[:scales]
    sum_ref, arrived_ref, table_ref, out_ref, new_out, turned, left, copy_sem = refs[scales:]
    lat_dev, padded, _ = sum_ref.shape
    chunk = out_ref.shape[2]
    depth = left.shape[2] // 2
    step = pl.program_id(0)

    def writes():
        return [pltpu.make_async_copy(ref, new_out.at[:, scale], copy_sem.at[scale]) for scale, ref in enumerate(new)]

    @pl.when(step == 0)
    def _():
        for copy in writes():
            copy.start()
        left[...] = jnp.zeros_like(left)
        turn_block(arrived_ref.at[arrived_ref.shape[0] - 1], group, turned, left, lat_dev, members)

    span = pl.ds(pl.multiple_of(step * chunk, chunk), chunk)
    values = left[...].reshape(lat_dev * padded, 2 * depth).astype(jnp.bfloat16)
    part = sum_ref[:, :, span] + contract(values, table_ref[: 3 * depth, span], depth).reshape(lat_dev, padded, chunk)
    out_ref[...] = part[:, :members, :]

    @pl.when(step == pl.num_programs(0) - 1)
    def _():
        for copy in writes():
            copy.wait()


def finish(new, summed, arrived, table):
    lat_dev, padded, length = summed.shape
    scales = len(new)
    slots, members, parts, width = new[0].shape
    group = plan(slots, lat_dev, members)[1]
    _, devices, rows, wide = arrived.shape
    depth = devices * rows
    chunk = 2 * LANES
    vmem = pl.BlockSpec(memory_space=pltpu.VMEM)
    return pl.pallas_call(
        functools.partial(finish_kernel, group, members, scales),
        grid=(length // chunk,),
        in_specs=[vmem] * (scales + 3),
        out_specs=[pl.BlockSpec((lat_dev, members, chunk), lambda n: (0, 0, n)), pl.BlockSpec(memory_space=pl.ANY)],
        out_shape=[
            jax.ShapeDtypeStruct((lat_dev, members, length), jnp.float32),
            jax.ShapeDtypeStruct((slots, scales, members, parts, width), jnp.float32),
        ],
        scratch_shapes=[
            pltpu.VMEM((wide, depth), jnp.float32),
            pltpu.VMEM((lat_dev, padded, 2 * depth), jnp.float32),
            pltpu.SemaphoreType.DMA((scales,)),
        ],
        compiler_params=pltpu.CompilerParams(dimension_semantics=("arbitrary",), vmem_limit_bytes=FINISH_LIMIT),
        name="finish",
    )(*[pltpu.with_memory_space_constraint(array, pltpu.VMEM) for array in (*new, summed, arrived, table)])


def local(coeffs_old, noise, legendre, decay, amplitude, wavenumber_of_slot, lat_order):
    slots, parts, scales, members, width = coeffs_old.shape
    length = 2 * legendre.shape[1]
    turn = (0, 2, 3, 1, 4)
    *new, summed, arrived, table = exchange(
        coeffs_old.transpose(turn), noise.transpose(turn), legendre, decay, amplitude, wavenumber_of_slot, lat_order, length
    )
    pattern, new = finish(new, summed, arrived, table)
    coeffs_new = new.transpose(0, 3, 1, 2, 4)
    return (coeffs_new, pattern)


def solution(mesh):
    split_rows = ("lat", "lon")
    in_specs = (
        P(split_rows, None, None, None, None),
        P(split_rows, None, None, None, None),
        P(split_rows, None, None),
        P(),
        P(),
        P(),
        P(),
    )
    out_specs = (P(split_rows, None, None, None, None), P(split_rows, None, None))
    return jax.shard_map(local, mesh=mesh, in_specs=in_specs, out_specs=out_specs, check_vma=False)
```

```python
import functools

import jax
import jax.numpy as jnp
from jax import lax
from jax.experimental import pallas as pl
from jax.experimental.pallas import tpu as pltpu
from jax.sharding import PartitionSpec as P

TWO_PI = 6.283185307179586
LANES = 128
SUBLANES = 8
HALF = 64
PARTS = 2
VMEM_LIMIT = 28 << 20
FINISH_LIMIT = 16 << 20
MESH = pl.DeviceIdType.MESH


def round_up(size, unit):
    return -(-size // unit) * unit


def split(x):
    high = x.astype(jnp.bfloat16)
    return high, (x - high.astype(jnp.float32)).astype(jnp.bfloat16)


class Group:
    def __init__(self, size, lat_dev, members):
        used = PARTS * size
        self.size = size
        self.fold = SUBLANES // used if SUBLANES % used == 0 and lat_dev % (SUBLANES // used) == 0 else 1
        self.rows = round_up(self.fold * used, SUBLANES)
        self.padded = self.rows > self.fold * used
        self.lat = lat_dev // self.fold
        self.wide = round_up(self.lat * members, LANES)

    def block(self, devices):
        return (devices, self.rows, self.wide)


def plan(slots, lat_dev, members):
    if slots % 4 == 0 and slots >= 8:
        sizes, size = (1, 1, 2), 4
    elif slots > 4:
        sizes, size = (slots % 4,), 4
    else:
        sizes, size = (), 1
    leaders = [Group(size_, lat_dev, members) for size_ in sizes]
    return leaders, Group(size, lat_dev, members), (slots - sum(sizes)) // size


def position():
    lat_size, lon_size = lax.axis_size("lat"), lax.axis_size("lon")
    return lax.axis_index("lat") * lon_size + lax.axis_index("lon"), lat_size * lon_size, lon_size


def turn_block(block_ref, group, turned, left, lat_dev, members):
    devices, rows, wide = block_ref.shape
    depth = devices * rows
    turned[:wide, :depth] = block_ref[...].reshape(depth, wide).T
    column = lax.broadcasted_iota(jnp.int32, (1, depth), 1)
    fold = lax.rem(column // (PARTS * group.size), group.fold)
    for q in range(lat_dev):
        start = members * (q % group.lat)
        piece = turned[start : start + members, :depth]
        if group.fold > 1:
            piece = jnp.where(fold == q // group.lat, piece, 0.0)
        high, low = split(piece)
        left[q, :members, :depth] = high.astype(jnp.float32)
        left[q, :members, depth : 2 * depth] = low.astype(jnp.float32)


def contract(values, table, depth):
    both = jnp.dot(values, table[: 2 * depth], preferred_element_type=jnp.float32)
    return both + jnp.dot(values[:, :depth], table[2 * depth :], preferred_element_type=jnp.float32)


def exchange_kernel(
    leaders, middle, count, members,
    order_hbm, waves_hbm, decay_hbm, amplitude_hbm, old_hbm, noise_hbm, basis_hbm,
    *refs,
):
    scales = old_hbm.shape[1]
    new = refs[:scales]
    (
        total, recv_middle, table,
        order_ref, waves_ref, decay_ref, amplitude_ref, small_sem,
        old, noise, basis, base_gains, gains, weights, field, send_lead, recv_lead, send_middle,
        wave, turned, left, load_sem, own_sem, send_sem, recv_sem,
    ) = refs[scales:]
    me, devices, lon_size = position()
    slots, lats, width = basis_hbm.shape
    lat_dev, padded, length = total.shape
    lead = len(leaders)
    starts = [sum(group.size for group in leaders[:index]) for index in range(lead + 1)]

    def peer(other):
        return other // lon_size, lax.rem(other, lon_size)

    def loads(slot):
        side = lax.rem(slot, 2)
        return (
            pltpu.make_async_copy(old_hbm.at[slot], old.at[side], load_sem.at[0, side]),
            pltpu.make_async_copy(noise_hbm.at[slot], noise.at[side], load_sem.at[1, side]),
            pltpu.make_async_copy(basis_hbm.at[slot], basis.at[side], load_sem.at[2, side]),
        )

    small = [
        pltpu.make_async_copy(source, target, small_sem.at[index])
        for index, (source, target) in enumerate(
            ((decay_hbm, decay_ref), (amplitude_hbm, amplitude_ref), (waves_hbm, waves_ref), (order_hbm, order_ref))
        )
    ]
    for copy in small:
        copy.start()
    for copy in loads(0):
        copy.start()
    barrier = pltpu.get_barrier_semaphore()

    def greet(k, carry):
        pl.semaphore_signal(barrier, inc=1, device_id=peer(lax.rem(me + k, devices)), device_id_type=MESH)
        return carry

    lax.fori_loop(1, devices, greet, 0)
    weights[...] = jnp.zeros_like(weights)
    base_gains[...] = jnp.zeros_like(base_gains)
    for copy in small:
        copy.wait()
    for scale in range(scales):
        decay = jnp.full((1, width), decay_ref[scale], jnp.float32)
        base_gains[scale : scale + 1, :] = amplitude_ref[scale : scale + 1, :] * jnp.sqrt(1.0 - decay * decay)
        base_gains[scales + scale : scales + scale + 1, :] = decay
    column = lax.broadcasted_iota(jnp.int32, (SUBLANES, width), 1)

    if any(group.padded for group in leaders + [middle]):
        field[...] = jnp.zeros_like(field)

    def transform(group, start):
        for inner in range(group.size):
            slot = start + inner

            @pl.when(slot + 1 < slots)
            def _():
                for copy in loads(slot + 1):
                    copy.start()

            old_load, noise_load, basis_load = loads(slot)
            old_load.wait()
            noise_load.wait()
            side = lax.rem(slot, 2)
            wave_here = waves_ref[me * slots + slot]
            gains[...] = jnp.where(column + wave_here < width, pltpu.roll(base_gains[...], width - wave_here, axis=1), 0.0)

            summed = None
            for scale in range(scales):
                fresh = gains[scale : scale + 1, :].reshape(1, 1, width)
                keep = gains[scales + scale : scales + scale + 1, :].reshape(1, 1, width)
                value = keep * old[side, scale] + fresh * noise[side, scale].astype(jnp.float32)
                new[scale][slot] = value
                summed = value if summed is None else summed + value
            for part in range(PARTS):
                weights[part * HALF : part * HALF + members, :] = summed[:, part, :]
            high, low = split(weights[...])
            basis_load.wait()
            basis_high, basis_low = split(basis[side])
            lanes = (((1,), (1,)), ((), ()))
            pair = lax.dot_general(basis_high, jnp.concatenate([high, low], axis=0), lanes, preferred_element_type=jnp.float32)
            small = lax.dot_general(basis_low, high, lanes, preferred_element_type=jnp.float32)
            product = pair[:, :LANES] + pair[:, LANES:] + small
            other = pltpu.roll(product, HALF, axis=1)
            for fold in range(group.fold):
                row = PARTS * (fold * group.size + inner)
                field[:, row, :] = product
                field[:, row + 1, :] = other

    def pack_and_send(group, send, recv, index):
        rows = group.rows
        lane = lax.broadcasted_iota(jnp.int32, (rows, LANES), 1)
        fold = lax.broadcasted_iota(jnp.int32, (rows, LANES), 0) // (PARTS * group.size)

        def remote(other):
            return pltpu.make_async_remote_copy(
                src_ref=send.at[other],
                dst_ref=recv.at[me],
                send_sem=send_sem.at[index],
                recv_sem=recv_sem.at[index],
                device_id=peer(other),
                device_id_type=MESH,
            )

        def one(k, carry):
            other = lax.rem(me + k, devices)
            tiles = [jnp.zeros((rows, LANES), jnp.float32) for _ in range(group.wide // LANES)]
            for q in range(lat_dev):
                piece = field[order_ref[other * lat_dev + q]][:rows]
                start = members * (q % group.lat)
                offset = start % LANES
                if offset:
                    piece = pltpu.roll(piece, offset, axis=1)
                tile = start // LANES
                keep = (lane >= offset) & (lane < offset + members)
                spill = lane < offset + members - LANES
                if group.fold > 1:
                    keep &= fold == q // group.lat
                    spill &= fold == q // group.lat
                tiles[tile] = jnp.where(keep, piece, tiles[tile])
                if offset + members > LANES:
                    tiles[tile + 1] = jnp.where(spill, piece, tiles[tile + 1])
            for position_, value in enumerate(tiles):
                send[other, :, position_ * LANES : (position_ + 1) * LANES] = value

            @pl.when(k == 1)
            def _():
                pltpu.make_async_copy(send.at[me], recv.at[me], own_sem.at[index]).start()

            @pl.when(k > 1)
            def _():
                remote(lax.rem(me + k - 1, devices)).start()

            return carry

        lax.fori_loop(0, devices, one, 0)
        remote(lax.rem(me + devices - 1, devices)).start()

    def await_group(recv, index):
        others = recv.at[pl.ds(0, devices - 1)]
        pltpu.make_async_copy(others, others, recv_sem.at[index]).wait()
        pltpu.make_async_copy(recv.at[0], recv.at[0], own_sem.at[index]).wait()

    for index, group in enumerate(leaders):
        transform(group, starts[index])
        if index == 0:
            pl.semaphore_wait(barrier, devices - 1)
        pack_and_send(group, send_lead[index], recv_lead[index], index)
    if not leaders:
        pl.semaphore_wait(barrier, devices - 1)

    def middle_step(step, carry):
        transform(middle, starts[lead] + step * middle.size)
        pack_and_send(middle, send_middle.at[step], recv_middle.at[step], step + lead)
        return carry

    lax.fori_loop(0, count, middle_step, 0)

    def make_table(group, start):
        rows = group.rows
        depth = devices * rows
        slot = lax.rem(lax.broadcasted_iota(jnp.int32, (rows, LANES), 0) // PARTS, group.size)

        def fill(device, carry):
            tile = jnp.zeros((rows, LANES), jnp.int32)
            for inner in range(group.size):
                tile = jnp.where(slot == inner, waves_ref[device * slots + start + inner], tile)
            wave[pl.ds(pl.multiple_of(device * rows, SUBLANES), rows), :] = tile.astype(jnp.float32)
            return carry

        lax.fori_loop(0, devices, fill, 0)
        waves = wave[:depth, :]
        lane = lax.broadcasted_iota(jnp.int32, (depth, LANES), 1).astype(jnp.float32)
        row = lax.broadcasted_iota(jnp.int32, (depth, LANES), 0)

        def angle(steps):
            turns = jnp.floor(steps * (1.0 / length))
            return (steps - turns * length) * (TWO_PI / length)

        base = angle(waves * lane) + jnp.where(lax.rem(row, PARTS) == 0, 0.0, TWO_PI / 4)
        weight = jnp.where(waves == 0.0, 1.0, 2.0)
        cosine, sine = weight * jnp.cos(base), weight * jnp.sin(base)
        stride = angle(waves * float(LANES))
        step_cosine, step_sine = jnp.cos(stride), jnp.sin(stride)
        for block in range(length // LANES):
            if block:
                cosine, sine = cosine * step_cosine - sine * step_sine, sine * step_cosine + cosine * step_sine
            high, low = split(cosine)
            span = slice(block * LANES, (block + 1) * LANES)
            table[:depth, span] = high
            table[depth : 2 * depth, span] = high
            table[2 * depth : 3 * depth, span] = low

    def synthesis(group, recv, index):
        depth = devices * group.rows
        await_group(recv, index)
        turn_block(recv, group, turned, left, lat_dev, members)
        values = left[:, :, : 2 * depth].reshape(lat_dev * padded, 2 * depth).astype(jnp.bfloat16)
        chunk = 2 * LANES

        def columns(n, carry):
            span = pl.ds(pl.multiple_of(n * chunk, chunk), chunk)
            total[:, :, span] += contract(values, table[: 3 * depth, span], depth).reshape(lat_dev, padded, chunk)
            return carry

        lax.fori_loop(0, length // chunk, columns, 0)

    left[...] = jnp.zeros_like(left)
    total[...] = jnp.zeros_like(total)
    for index, group in enumerate(leaders):
        make_table(group, starts[index])
        synthesis(group, recv_lead[index], index)

    def middle_synthesis(step, carry):
        make_table(middle, starts[lead] + step * middle.size)

        @pl.when(step < count - 1)
        def _():
            synthesis(middle, recv_middle.at[step], step + lead)

        return carry

    lax.fori_loop(0, count, middle_synthesis, 0)

    def sent(block, index):
        others = block.at[pl.ds(0, devices - 1)]
        pltpu.make_async_copy(others, others, send_sem.at[index]).wait()

    for index in range(lead):
        sent(send_lead[index], index)

    def middle_sent(step, carry):
        sent(send_middle.at[step], step + lead)
        return carry

    lax.fori_loop(0, count, middle_sent, 0)
    await_group(recv_middle.at[count - 1], lead + count - 1)


def exchange(old, noise, legendre, decay, amplitude, waves, lat_order, length):
    devices = lax.axis_size("lat") * lax.axis_size("lon")
    slots, scales, members, parts, width = old.shape
    lats = legendre.shape[1]
    lat_dev = lats // devices
    leaders, middle, count = plan(slots, lat_dev, members)
    groups = leaders + [middle]
    lead_blocks = tuple(pltpu.VMEM(group.block(devices), jnp.float32) for group in leaders)
    padded = round_up(members, SUBLANES)
    rows = max(group.rows for group in groups)
    depth = devices * rows
    vmem = pl.BlockSpec(memory_space=pltpu.VMEM)
    hbm = pl.BlockSpec(memory_space=pltpu.HBM)
    operands = (lat_order, waves, decay, amplitude, old, noise, legendre)
    operands = [pltpu.with_memory_space_constraint(array, pltpu.HBM) for array in operands]
    return pl.pallas_call(
        functools.partial(exchange_kernel, leaders, middle, count, members),
        in_specs=[hbm] * len(operands),
        out_specs=[vmem] * (scales + 3),
        out_shape=[pltpu.VMEM((slots, members, parts, width), jnp.float32)] * scales
        + [
            pltpu.VMEM((lat_dev, padded, length), jnp.float32),
            pltpu.VMEM((count,) + middle.block(devices), jnp.float32),
            pltpu.VMEM((3 * depth, length), jnp.bfloat16),
        ],
        scratch_shapes=[
            pltpu.SMEM(lat_order.shape, jnp.int32),
            pltpu.SMEM(waves.shape, jnp.int32),
            pltpu.SMEM(decay.shape, jnp.float32),
            pltpu.VMEM(amplitude.shape, jnp.float32),
            pltpu.SemaphoreType.DMA((4,)),
            pltpu.VMEM((2, scales, members, parts, width), jnp.float32),
            pltpu.VMEM((2, scales, members, parts, width), jnp.bfloat16),
            pltpu.VMEM((2, lats, width), jnp.float32),
            pltpu.VMEM((SUBLANES, width), jnp.float32),
            pltpu.VMEM((SUBLANES, width), jnp.float32),
            pltpu.VMEM((LANES, width), jnp.float32),
            pltpu.VMEM((lats, rows, LANES), jnp.float32),
            lead_blocks,
            lead_blocks,
            pltpu.VMEM((count,) + middle.block(devices), jnp.float32),
            pltpu.VMEM((depth, LANES), jnp.float32),
            pltpu.VMEM((max(group.wide for group in groups), depth), jnp.float32),
            pltpu.VMEM((lat_dev, padded, 2 * depth), jnp.float32),
            pltpu.SemaphoreType.DMA((3, 2)),
            pltpu.SemaphoreType.DMA((len(leaders) + count,)),
            pltpu.SemaphoreType.DMA((len(leaders) + count,)),
            pltpu.SemaphoreType.DMA((len(leaders) + count,)),
        ],
        compiler_params=pltpu.CompilerParams(collective_id=0, has_side_effects=True, vmem_limit_bytes=VMEM_LIMIT),
        name="exchange",
    )(*operands)


def finish_kernel(group, members, scales, *refs):
    new = refs[:scales]
    sum_ref, arrived_ref, table_ref, out_ref, new_out, turned, left, copy_sem = refs[scales:]
    lat_dev, padded, length = sum_ref.shape
    chunk = out_ref.shape[2]
    depth = left.shape[2] // 2
    step = pl.program_id(0)

    slots = new_out.shape[0]
    share = -(-slots // (length // chunk - 1))

    def write(slot, carry):
        for scale, ref in enumerate(new):
            pltpu.make_async_copy(ref.at[slot], new_out.at[slot, scale], copy_sem.at[scale]).start()
        return carry

    lax.fori_loop(jnp.minimum(share * step, slots), jnp.minimum(share * (step + 1), slots), write, 0)

    @pl.when(step == 0)
    def _():
        left[...] = jnp.zeros_like(left)
        turn_block(arrived_ref.at[arrived_ref.shape[0] - 1], group, turned, left, lat_dev, members)

    span = pl.ds(pl.multiple_of(step * chunk, chunk), chunk)
    values = left[...].reshape(lat_dev * padded, 2 * depth).astype(jnp.bfloat16)
    part = sum_ref[:, :, span] + contract(values, table_ref[: 3 * depth, span], depth).reshape(lat_dev, padded, chunk)
    out_ref[...] = part[:, :members, :]

    @pl.when(step == pl.num_programs(0) - 1)
    def _():
        for scale, ref in enumerate(new):
            pltpu.make_async_copy(ref, new_out.at[:, scale], copy_sem.at[scale]).wait()


def finish(new, summed, arrived, table):
    lat_dev, padded, length = summed.shape
    scales = len(new)
    slots, members, parts, width = new[0].shape
    group = plan(slots, lat_dev, members)[1]
    _, devices, rows, wide = arrived.shape
    depth = devices * rows
    chunk = 2 * LANES
    vmem = pl.BlockSpec(memory_space=pltpu.VMEM)
    return pl.pallas_call(
        functools.partial(finish_kernel, group, members, scales),
        grid=(length // chunk,),
        in_specs=[vmem] * (scales + 3),
        out_specs=[pl.BlockSpec((lat_dev, members, chunk), lambda n: (0, 0, n)), pl.BlockSpec(memory_space=pl.ANY)],
        out_shape=[
            jax.ShapeDtypeStruct((lat_dev, members, length), jnp.float32),
            jax.ShapeDtypeStruct((slots, scales, members, parts, width), jnp.float32),
        ],
        scratch_shapes=[
            pltpu.VMEM((wide, depth), jnp.float32),
            pltpu.VMEM((lat_dev, padded, 2 * depth), jnp.float32),
            pltpu.SemaphoreType.DMA((scales,)),
        ],
        compiler_params=pltpu.CompilerParams(dimension_semantics=("arbitrary",), vmem_limit_bytes=FINISH_LIMIT),
        name="finish",
    )(*[pltpu.with_memory_space_constraint(array, pltpu.VMEM) for array in (*new, summed, arrived, table)])


def local(coeffs_old, noise, legendre, decay, amplitude, wavenumber_of_slot, lat_order):
    slots, parts, scales, members, width = coeffs_old.shape
    length = 2 * legendre.shape[1]
    turn = (0, 2, 3, 1, 4)
    *new, summed, arrived, table = exchange(
        coeffs_old.transpose(turn), noise.transpose(turn), legendre, decay, amplitude, wavenumber_of_slot, lat_order, length
    )
    pattern, new = finish(new, summed, arrived, table)
    coeffs_new = new.transpose(0, 3, 1, 2, 4)
    return (coeffs_new, pattern)


def solution(mesh):
    split_rows = ("lat", "lon")
    in_specs = (
        P(split_rows, None, None, None, None),
        P(split_rows, None, None, None, None),
        P(split_rows, None, None),
        P(),
        P(),
        P(),
        P(),
    )
    out_specs = (P(split_rows, None, None, None, None), P(split_rows, None, None))
    return jax.shard_map(local, mesh=mesh, in_specs=in_specs, out_specs=out_specs, check_vma=False)
```

```python
import functools

import jax
import jax.numpy as jnp
from jax import lax
from jax.experimental import pallas as pl
from jax.experimental.pallas import tpu as pltpu
from jax.sharding import PartitionSpec as P

TWO_PI = 6.283185307179586
LANES = 128
SUBLANES = 8
HALF = 64
PARTS = 2
VMEM_LIMIT = 28 << 20
FINISH_LIMIT = 16 << 20
MESH = pl.DeviceIdType.MESH


def round_up(size, unit):
    return -(-size // unit) * unit


def split(x):
    high = x.astype(jnp.bfloat16)
    return high, (x - high.astype(jnp.float32)).astype(jnp.bfloat16)


class Group:
    def __init__(self, size, lat_dev, members):
        used = PARTS * size
        self.size = size
        self.fold = SUBLANES // used if SUBLANES % used == 0 and lat_dev % (SUBLANES // used) == 0 else 1
        self.rows = round_up(self.fold * used, SUBLANES)
        self.padded = self.rows > self.fold * used
        self.lat = lat_dev // self.fold
        self.wide = round_up(self.lat * members, LANES)

    def block(self, devices):
        return (devices, self.rows, self.wide)


def plan(slots, lat_dev, members):
    if slots % 4 == 0 and slots >= 8:
        sizes, size = (1, 1, 2), 4
    elif slots > 4:
        sizes, size = (slots % 4,), 4
    else:
        sizes, size = (), 1
    leaders = [Group(size_, lat_dev, members) for size_ in sizes]
    return leaders, Group(size, lat_dev, members), (slots - sum(sizes)) // size


def position():
    lat_size, lon_size = lax.axis_size("lat"), lax.axis_size("lon")
    return lax.axis_index("lat") * lon_size + lax.axis_index("lon"), lat_size * lon_size, lon_size


def turn_block(block_ref, group, turned, left, lat_dev, members):
    devices, rows, wide = block_ref.shape
    depth = devices * rows
    turned[:wide, :depth] = block_ref[...].reshape(depth, wide).T
    column = lax.broadcasted_iota(jnp.int32, (1, depth), 1)
    fold = lax.rem(column // (PARTS * group.size), group.fold)
    for q in range(lat_dev):
        start = members * (q % group.lat)
        piece = turned[start : start + members, :depth]
        if group.fold > 1:
            piece = jnp.where(fold == q // group.lat, piece, 0.0)
        high, low = split(piece)
        left[q, :members, :depth] = high.astype(jnp.float32)
        left[q, :members, depth : 2 * depth] = low.astype(jnp.float32)


def contract(values, table, depth):
    both = jnp.dot(values, table[: 2 * depth], preferred_element_type=jnp.float32)
    return both + jnp.dot(values[:, :depth], table[2 * depth :], preferred_element_type=jnp.float32)


def exchange_kernel(
    leaders, middle, count, members,
    order_hbm, waves_hbm, decay_hbm, amplitude_hbm, old_hbm, noise_hbm, basis_hbm,
    *refs,
):
    scales = old_hbm.shape[1]
    new = refs[:scales]
    (
        total, recv_middle, table,
        order_ref, waves_ref, decay_ref, amplitude_ref, small_sem,
        old, noise, basis, base_gains, gains, weights, field, send_lead, recv_lead, send_middle,
        wave, turned, left, load_sem, own_sem, send_sem, recv_sem,
    ) = refs[scales:]
    me, devices, lon_size = position()
    slots, lats, width = basis_hbm.shape
    lat_dev, padded, length = total.shape
    lead = len(leaders)
    starts = [sum(group.size for group in leaders[:index]) for index in range(lead + 1)]

    def peer(other):
        return other // lon_size, lax.rem(other, lon_size)

    def loads(slot):
        side = lax.rem(slot, 2)
        return (
            pltpu.make_async_copy(old_hbm.at[slot], old.at[side], load_sem.at[0, side]),
            pltpu.make_async_copy(noise_hbm.at[slot], noise.at[side], load_sem.at[1, side]),
            pltpu.make_async_copy(basis_hbm.at[slot], basis.at[side], load_sem.at[2, side]),
        )

    small = [
        pltpu.make_async_copy(source, target, small_sem.at[index])
        for index, (source, target) in enumerate(
            ((decay_hbm, decay_ref), (amplitude_hbm, amplitude_ref), (waves_hbm, waves_ref), (order_hbm, order_ref))
        )
    ]
    for copy in small:
        copy.start()
    for copy in loads(0):
        copy.start()
    barrier = pltpu.get_barrier_semaphore()

    def greet(k, carry):
        pl.semaphore_signal(barrier, inc=1, device_id=peer(lax.rem(me + k, devices)), device_id_type=MESH)
        return carry

    lax.fori_loop(1, devices, greet, 0)
    weights[...] = jnp.zeros_like(weights)
    base_gains[...] = jnp.zeros_like(base_gains)
    for copy in small:
        copy.wait()
    for scale in range(scales):
        decay = jnp.full((1, width), decay_ref[scale], jnp.float32)
        base_gains[scale : scale + 1, :] = amplitude_ref[scale : scale + 1, :] * jnp.sqrt(1.0 - decay * decay)
        base_gains[scales + scale : scales + scale + 1, :] = decay
    column = lax.broadcasted_iota(jnp.int32, (SUBLANES, width), 1)

    if any(group.padded for group in leaders + [middle]):
        field[...] = jnp.zeros_like(field)

    def transform(group, start):
        for inner in range(group.size):
            slot = start + inner

            @pl.when(slot + 1 < slots)
            def _():
                for copy in loads(slot + 1):
                    copy.start()

            for copy in loads(slot):
                copy.wait()
            side = lax.rem(slot, 2)
            wave_here = waves_ref[me * slots + slot]
            gains[...] = jnp.where(column + wave_here < width, pltpu.roll(base_gains[...], width - wave_here, axis=1), 0.0)

            summed = None
            for scale in range(scales):
                fresh = gains[scale : scale + 1, :].reshape(1, 1, width)
                keep = gains[scales + scale : scales + scale + 1, :].reshape(1, 1, width)
                value = keep * old[side, scale] + fresh * noise[side, scale].astype(jnp.float32)
                new[scale][slot] = value
                summed = value if summed is None else summed + value
            for part in range(PARTS):
                weights[part * HALF : part * HALF + members, :] = summed[:, part, :]
            high, low = split(weights[...])
            basis_high, basis_low = split(basis[side])
            lanes = (((1,), (1,)), ((), ()))
            pair = lax.dot_general(basis_high, jnp.concatenate([high, low], axis=0), lanes, preferred_element_type=jnp.float32)
            small = lax.dot_general(basis_low, high, lanes, preferred_element_type=jnp.float32)
            product = pair[:, :LANES] + pair[:, LANES:] + small
            other = pltpu.roll(product, HALF, axis=1)
            for fold in range(group.fold):
                row = PARTS * (fold * group.size + inner)
                field[:, row, :] = product
                field[:, row + 1, :] = other

    def pack_and_send(group, send, recv, index):
        rows = group.rows
        lane = lax.broadcasted_iota(jnp.int32, (rows, LANES), 1)
        fold = lax.broadcasted_iota(jnp.int32, (rows, LANES), 0) // (PARTS * group.size)

        def remote(other):
            return pltpu.make_async_remote_copy(
                src_ref=send.at[other],
                dst_ref=recv.at[me],
                send_sem=send_sem.at[index],
                recv_sem=recv_sem.at[index],
                device_id=peer(other),
                device_id_type=MESH,
            )

        def one(k, carry):
            other = lax.rem(me + k, devices)
            tiles = [jnp.zeros((rows, LANES), jnp.float32) for _ in range(group.wide // LANES)]
            for q in range(lat_dev):
                piece = field[order_ref[other * lat_dev + q]][:rows]
                start = members * (q % group.lat)
                offset = start % LANES
                if offset:
                    piece = pltpu.roll(piece, offset, axis=1)
                tile = start // LANES
                keep = (lane >= offset) & (lane < offset + members)
                spill = lane < offset + members - LANES
                if group.fold > 1:
                    keep &= fold == q // group.lat
                    spill &= fold == q // group.lat
                tiles[tile] = jnp.where(keep, piece, tiles[tile])
                if offset + members > LANES:
                    tiles[tile + 1] = jnp.where(spill, piece, tiles[tile + 1])
            for position_, value in enumerate(tiles):
                send[other, :, position_ * LANES : (position_ + 1) * LANES] = value

            @pl.when(k == 1)
            def _():
                pltpu.make_async_copy(send.at[me], recv.at[me], own_sem.at[index]).start()

            @pl.when(k > 1)
            def _():
                remote(lax.rem(me + k - 1, devices)).start()

            return carry

        lax.fori_loop(0, devices, one, 0)
        remote(lax.rem(me + devices - 1, devices)).start()

    def await_group(recv, index):
        others = recv.at[pl.ds(0, devices - 1)]
        pltpu.make_async_copy(others, others, recv_sem.at[index]).wait()
        pltpu.make_async_copy(recv.at[0], recv.at[0], own_sem.at[index]).wait()

    for index, group in enumerate(leaders):
        transform(group, starts[index])
        if index == 0:
            pl.semaphore_wait(barrier, devices - 1)
        pack_and_send(group, send_lead[index], recv_lead[index], index)
    if not leaders:
        pl.semaphore_wait(barrier, devices - 1)

    def middle_step(step, carry):
        transform(middle, starts[lead] + step * middle.size)
        pack_and_send(middle, send_middle.at[step], recv_middle.at[step], step + lead)
        return carry

    lax.fori_loop(0, count, middle_step, 0)

    def make_table(group, start):
        rows = group.rows
        depth = devices * rows
        slot = lax.rem(lax.broadcasted_iota(jnp.int32, (rows, LANES), 0) // PARTS, group.size)

        def fill(device, carry):
            tile = jnp.zeros((rows, LANES), jnp.int32)
            for inner in range(group.size):
                tile = jnp.where(slot == inner, waves_ref[device * slots + start + inner], tile)
            wave[pl.ds(pl.multiple_of(device * rows, SUBLANES), rows), :] = tile.astype(jnp.float32)
            return carry

        lax.fori_loop(0, devices, fill, 0)
        waves = wave[:depth, :]
        lane = lax.broadcasted_iota(jnp.int32, (depth, LANES), 1).astype(jnp.float32)
        row = lax.broadcasted_iota(jnp.int32, (depth, LANES), 0)

        def angle(steps):
            turns = jnp.floor(steps * (1.0 / length))
            return (steps - turns * length) * (TWO_PI / length)

        base = angle(waves * lane) + jnp.where(lax.rem(row, PARTS) == 0, 0.0, TWO_PI / 4)
        weight = jnp.where(waves == 0.0, 1.0, 2.0)
        cosine, sine = weight * jnp.cos(base), weight * jnp.sin(base)
        stride = angle(waves * float(LANES))
        step_cosine, step_sine = jnp.cos(stride), jnp.sin(stride)
        for block in range(length // LANES):
            if block:
                cosine, sine = cosine * step_cosine - sine * step_sine, sine * step_cosine + cosine * step_sine
            high, low = split(cosine)
            span = slice(block * LANES, (block + 1) * LANES)
            table[:depth, span] = high
            table[depth : 2 * depth, span] = high
            table[2 * depth : 3 * depth, span] = low

    def synthesis(group, recv, index):
        depth = devices * group.rows
        await_group(recv, index)
        turn_block(recv, group, turned, left, lat_dev, members)
        values = left[:, :, : 2 * depth].reshape(lat_dev * padded, 2 * depth).astype(jnp.bfloat16)
        chunk = 2 * LANES

        def columns(n, carry):
            span = pl.ds(pl.multiple_of(n * chunk, chunk), chunk)
            total[:, :, span] += contract(values, table[: 3 * depth, span], depth).reshape(lat_dev, padded, chunk)
            return carry

        lax.fori_loop(0, length // chunk, columns, 0)

    left[...] = jnp.zeros_like(left)
    total[...] = jnp.zeros_like(total)
    for index, group in enumerate(leaders):
        make_table(group, starts[index])
        synthesis(group, recv_lead[index], index)

    def middle_synthesis(step, carry):
        make_table(middle, starts[lead] + step * middle.size)

        @pl.when(step < count - 1)
        def _():
            synthesis(middle, recv_middle.at[step], step + lead)

        return carry

    lax.fori_loop(0, count, middle_synthesis, 0)

    def sent(block, index):
        others = block.at[pl.ds(0, devices - 1)]
        pltpu.make_async_copy(others, others, send_sem.at[index]).wait()

    for index in range(lead):
        sent(send_lead[index], index)

    def middle_sent(step, carry):
        sent(send_middle.at[step], step + lead)
        return carry

    lax.fori_loop(0, count, middle_sent, 0)
    await_group(recv_middle.at[count - 1], lead + count - 1)


def exchange(old, noise, legendre, decay, amplitude, waves, lat_order, length):
    devices = lax.axis_size("lat") * lax.axis_size("lon")
    slots, scales, members, parts, width = old.shape
    lats = legendre.shape[1]
    lat_dev = lats // devices
    leaders, middle, count = plan(slots, lat_dev, members)
    groups = leaders + [middle]
    lead_blocks = tuple(pltpu.VMEM(group.block(devices), jnp.float32) for group in leaders)
    padded = round_up(members, SUBLANES)
    rows = max(group.rows for group in groups)
    depth = devices * rows
    vmem = pl.BlockSpec(memory_space=pltpu.VMEM)
    hbm = pl.BlockSpec(memory_space=pltpu.HBM)
    operands = (lat_order, waves, decay, amplitude, old, noise, legendre)
    operands = [pltpu.with_memory_space_constraint(array, pltpu.HBM) for array in operands]
    return pl.pallas_call(
        functools.partial(exchange_kernel, leaders, middle, count, members),
        in_specs=[hbm] * len(operands),
        out_specs=[vmem] * (scales + 3),
        out_shape=[pltpu.VMEM((slots, members, parts, width), jnp.float32)] * scales
        + [
            pltpu.VMEM((lat_dev, padded, length), jnp.float32),
            pltpu.VMEM((count,) + middle.block(devices), jnp.float32),
            pltpu.VMEM((3 * depth, length), jnp.bfloat16),
        ],
        scratch_shapes=[
            pltpu.SMEM(lat_order.shape, jnp.int32),
            pltpu.SMEM(waves.shape, jnp.int32),
            pltpu.SMEM(decay.shape, jnp.float32),
            pltpu.VMEM(amplitude.shape, jnp.float32),
            pltpu.SemaphoreType.DMA((4,)),
            pltpu.VMEM((2, scales, members, parts, width), jnp.float32),
            pltpu.VMEM((2, scales, members, parts, width), jnp.bfloat16),
            pltpu.VMEM((2, lats, width), jnp.float32),
            pltpu.VMEM((SUBLANES, width), jnp.float32),
            pltpu.VMEM((SUBLANES, width), jnp.float32),
            pltpu.VMEM((LANES, width), jnp.float32),
            pltpu.VMEM((lats, rows, LANES), jnp.float32),
            lead_blocks,
            lead_blocks,
            pltpu.VMEM((count,) + middle.block(devices), jnp.float32),
            pltpu.VMEM((depth, LANES), jnp.float32),
            pltpu.VMEM((max(group.wide for group in groups), depth), jnp.float32),
            pltpu.VMEM((lat_dev, padded, 2 * depth), jnp.float32),
            pltpu.SemaphoreType.DMA((3, 2)),
            pltpu.SemaphoreType.DMA((len(leaders) + count,)),
            pltpu.SemaphoreType.DMA((len(leaders) + count,)),
            pltpu.SemaphoreType.DMA((len(leaders) + count,)),
        ],
        compiler_params=pltpu.CompilerParams(collective_id=0, has_side_effects=True, vmem_limit_bytes=VMEM_LIMIT),
        name="exchange",
    )(*operands)


def finish_kernel(group, members, scales, *refs):
    new = refs[:scales]
    sum_ref, arrived_ref, table_ref, out_ref, new_out, turned, left, copy_sem = refs[scales:]
    lat_dev, padded, length = sum_ref.shape
    chunk = out_ref.shape[2]
    depth = left.shape[2] // 2
    step = pl.program_id(0)

    slots = new_out.shape[0]
    share = -(-slots // (length // chunk - 1))

    def write(slot, carry):
        for scale, ref in enumerate(new):
            pltpu.make_async_copy(ref.at[slot], new_out.at[slot, scale], copy_sem.at[scale]).start()
        return carry

    lax.fori_loop(jnp.minimum(share * step, slots), jnp.minimum(share * (step + 1), slots), write, 0)

    @pl.when(step == 0)
    def _():
        left[...] = jnp.zeros_like(left)
        turn_block(arrived_ref.at[arrived_ref.shape[0] - 1], group, turned, left, lat_dev, members)

    span = pl.ds(pl.multiple_of(step * chunk, chunk), chunk)
    values = left[...].reshape(lat_dev * padded, 2 * depth).astype(jnp.bfloat16)
    part = sum_ref[:, :, span] + contract(values, table_ref[: 3 * depth, span], depth).reshape(lat_dev, padded, chunk)
    out_ref[...] = part[:, :members, :]

    @pl.when(step == pl.num_programs(0) - 1)
    def _():
        for scale, ref in enumerate(new):
            pltpu.make_async_copy(ref, new_out.at[:, scale], copy_sem.at[scale]).wait()


def finish(new, summed, arrived, table):
    lat_dev, padded, length = summed.shape
    scales = len(new)
    slots, members, parts, width = new[0].shape
    group = plan(slots, lat_dev, members)[1]
    _, devices, rows, wide = arrived.shape
    depth = devices * rows
    chunk = 2 * LANES
    vmem = pl.BlockSpec(memory_space=pltpu.VMEM)
    return pl.pallas_call(
        functools.partial(finish_kernel, group, members, scales),
        grid=(length // chunk,),
        in_specs=[vmem] * (scales + 3),
        out_specs=[pl.BlockSpec((lat_dev, members, chunk), lambda n: (0, 0, n)), pl.BlockSpec(memory_space=pl.ANY)],
        out_shape=[
            jax.ShapeDtypeStruct((lat_dev, members, length), jnp.float32),
            jax.ShapeDtypeStruct((slots, scales, members, parts, width), jnp.float32),
        ],
        scratch_shapes=[
            pltpu.VMEM((wide, depth), jnp.float32),
            pltpu.VMEM((lat_dev, padded, 2 * depth), jnp.float32),
            pltpu.SemaphoreType.DMA((scales,)),
        ],
        compiler_params=pltpu.CompilerParams(dimension_semantics=("arbitrary",), vmem_limit_bytes=FINISH_LIMIT),
        name="finish",
    )(*[pltpu.with_memory_space_constraint(array, pltpu.VMEM) for array in (*new, summed, arrived, table)])


def local(coeffs_old, noise, legendre, decay, amplitude, wavenumber_of_slot, lat_order):
    slots, parts, scales, members, width = coeffs_old.shape
    length = 2 * legendre.shape[1]
    turn = (0, 2, 3, 1, 4)
    *new, summed, arrived, table = exchange(
        coeffs_old.transpose(turn), noise.transpose(turn), legendre, decay, amplitude, wavenumber_of_slot, lat_order, length
    )
    pattern, new = finish(new, summed, arrived, table)
    coeffs_new = new.transpose(0, 3, 1, 2, 4)
    return (coeffs_new, pattern)


def solution(mesh):
    split_rows = ("lat", "lon")
    in_specs = (
        P(split_rows, None, None, None, None),
        P(split_rows, None, None, None, None),
        P(split_rows, None, None),
        P(),
        P(),
        P(),
        P(),
    )
    out_specs = (P(split_rows, None, None, None, None), P(split_rows, None, None))
    return jax.shard_map(local, mesh=mesh, in_specs=in_specs, out_specs=out_specs, check_vma=False)
```

```python
import functools

import jax
import jax.numpy as jnp
from jax import lax
from jax.experimental import pallas as pl
from jax.experimental.pallas import tpu as pltpu
from jax.sharding import PartitionSpec as P

TWO_PI = 6.283185307179586
LANES = 128
SUBLANES = 8
HALF = 64
PARTS = 2
VMEM_LIMIT = 28 << 20
FINISH_LIMIT = 16 << 20
MESH = pl.DeviceIdType.MESH


def round_up(size, unit):
    return -(-size // unit) * unit


def split(x):
    high = x.astype(jnp.bfloat16)
    return high, (x - high.astype(jnp.float32)).astype(jnp.bfloat16)


class Group:
    def __init__(self, size, lat_dev, members):
        used = PARTS * size
        self.size = size
        self.fold = SUBLANES // used if SUBLANES % used == 0 and lat_dev % (SUBLANES // used) == 0 else 1
        self.rows = round_up(self.fold * used, SUBLANES)
        self.padded = self.rows > self.fold * used
        self.lat = lat_dev // self.fold
        self.wide = round_up(self.lat * members, LANES)

    def block(self, devices):
        return (devices, self.rows, self.wide)


def plan(slots, lat_dev, members):
    if slots % 4 == 0 and slots >= 8:
        sizes, size = (2, 2), 4
    elif slots > 4:
        sizes, size = (slots % 4,), 4
    else:
        sizes, size = (), 1
    leaders = [Group(size_, lat_dev, members) for size_ in sizes]
    return leaders, Group(size, lat_dev, members), (slots - sum(sizes)) // size


def position():
    lat_size, lon_size = lax.axis_size("lat"), lax.axis_size("lon")
    return lax.axis_index("lat") * lon_size + lax.axis_index("lon"), lat_size * lon_size, lon_size


def turn_block(block_ref, group, turned, left, lat_dev, members):
    devices, rows, wide = block_ref.shape
    depth = devices * rows
    turned[:wide, :depth] = block_ref[...].reshape(depth, wide).T
    column = lax.broadcasted_iota(jnp.int32, (1, depth), 1)
    fold = lax.rem(column // (PARTS * group.size), group.fold)
    for q in range(lat_dev):
        start = members * (q % group.lat)
        piece = turned[start : start + members, :depth]
        if group.fold > 1:
            piece = jnp.where(fold == q // group.lat, piece, 0.0)
        high, low = split(piece)
        left[q, :members, :depth] = high.astype(jnp.float32)
        left[q, :members, depth : 2 * depth] = low.astype(jnp.float32)


def contract(values, table, depth):
    both = jnp.dot(values, table[: 2 * depth], preferred_element_type=jnp.float32)
    return both + jnp.dot(values[:, :depth], table[2 * depth :], preferred_element_type=jnp.float32)


def exchange_kernel(
    leaders, middle, count, members,
    order_hbm, waves_hbm, decay_hbm, amplitude_hbm, old_hbm, noise_hbm, basis_hbm,
    *refs,
):
    scales = old_hbm.shape[1]
    new = refs[:scales]
    (
        total, recv_middle, table,
        order_ref, waves_ref, decay_ref, amplitude_ref, small_sem,
        old, noise, basis, base_gains, gains, weights, field, send_lead, recv_lead, send_middle,
        wave, turned, left, load_sem, own_sem, send_sem, recv_sem,
    ) = refs[scales:]
    me, devices, lon_size = position()
    slots, lats, width = basis_hbm.shape
    lat_dev, padded, length = total.shape
    lead = len(leaders)
    starts = [sum(group.size for group in leaders[:index]) for index in range(lead + 1)]

    def peer(other):
        return other // lon_size, lax.rem(other, lon_size)

    def loads(slot):
        side = lax.rem(slot, 2)
        return (
            pltpu.make_async_copy(old_hbm.at[slot], old.at[side], load_sem.at[0, side]),
            pltpu.make_async_copy(noise_hbm.at[slot], noise.at[side], load_sem.at[1, side]),
            pltpu.make_async_copy(basis_hbm.at[slot], basis.at[side], load_sem.at[2, side]),
        )

    small = [
        pltpu.make_async_copy(source, target, small_sem.at[index])
        for index, (source, target) in enumerate(
            ((decay_hbm, decay_ref), (amplitude_hbm, amplitude_ref), (waves_hbm, waves_ref), (order_hbm, order_ref))
        )
    ]
    for copy in small:
        copy.start()
    for copy in loads(0):
        copy.start()
    barrier = pltpu.get_barrier_semaphore()

    def greet(k, carry):
        pl.semaphore_signal(barrier, inc=1, device_id=peer(lax.rem(me + k, devices)), device_id_type=MESH)
        return carry

    lax.fori_loop(1, devices, greet, 0)
    weights[...] = jnp.zeros_like(weights)
    base_gains[...] = jnp.zeros_like(base_gains)
    for copy in small:
        copy.wait()
    for scale in range(scales):
        decay = jnp.full((1, width), decay_ref[scale], jnp.float32)
        base_gains[scale : scale + 1, :] = amplitude_ref[scale : scale + 1, :] * jnp.sqrt(1.0 - decay * decay)
        base_gains[scales + scale : scales + scale + 1, :] = decay
    column = lax.broadcasted_iota(jnp.int32, (SUBLANES, width), 1)

    if any(group.padded for group in leaders + [middle]):
        field[...] = jnp.zeros_like(field)

    def transform(group, start):
        for inner in range(group.size):
            slot = start + inner

            @pl.when(slot + 1 < slots)
            def _():
                for copy in loads(slot + 1):
                    copy.start()

            for copy in loads(slot):
                copy.wait()
            side = lax.rem(slot, 2)
            wave_here = waves_ref[me * slots + slot]
            gains[...] = jnp.where(column + wave_here < width, pltpu.roll(base_gains[...], width - wave_here, axis=1), 0.0)

            summed = None
            for scale in range(scales):
                fresh = gains[scale : scale + 1, :].reshape(1, 1, width)
                keep = gains[scales + scale : scales + scale + 1, :].reshape(1, 1, width)
                value = keep * old[side, scale] + fresh * noise[side, scale].astype(jnp.float32)
                new[scale][slot] = value
                summed = value if summed is None else summed + value
            for part in range(PARTS):
                weights[part * HALF : part * HALF + members, :] = summed[:, part, :]
            high, low = split(weights[...])
            basis_high, basis_low = split(basis[side])
            lanes = (((1,), (1,)), ((), ()))
            pair = lax.dot_general(basis_high, jnp.concatenate([high, low], axis=0), lanes, preferred_element_type=jnp.float32)
            small = lax.dot_general(basis_low, high, lanes, preferred_element_type=jnp.float32)
            product = pair[:, :LANES] + pair[:, LANES:] + small
            other = pltpu.roll(product, HALF, axis=1)
            for fold in range(group.fold):
                row = PARTS * (fold * group.size + inner)
                field[:, row, :] = product
                field[:, row + 1, :] = other

    def pack_and_send(group, send, recv, index):
        rows = group.rows
        lane = lax.broadcasted_iota(jnp.int32, (rows, LANES), 1)
        fold = lax.broadcasted_iota(jnp.int32, (rows, LANES), 0) // (PARTS * group.size)

        def remote(other):
            return pltpu.make_async_remote_copy(
                src_ref=send.at[other],
                dst_ref=recv.at[me],
                send_sem=send_sem.at[index],
                recv_sem=recv_sem.at[index],
                device_id=peer(other),
                device_id_type=MESH,
            )

        def one(k, carry):
            other = lax.rem(me + k, devices)
            tiles = [jnp.zeros((rows, LANES), jnp.float32) for _ in range(group.wide // LANES)]
            for q in range(lat_dev):
                piece = field[order_ref[other * lat_dev + q]][:rows]
                start = members * (q % group.lat)
                offset = start % LANES
                if offset:
                    piece = pltpu.roll(piece, offset, axis=1)
                tile = start // LANES
                keep = (lane >= offset) & (lane < offset + members)
                spill = lane < offset + members - LANES
                if group.fold > 1:
                    keep &= fold == q // group.lat
                    spill &= fold == q // group.lat
                tiles[tile] = jnp.where(keep, piece, tiles[tile])
                if offset + members > LANES:
                    tiles[tile + 1] = jnp.where(spill, piece, tiles[tile + 1])
            for position_, value in enumerate(tiles):
                send[other, :, position_ * LANES : (position_ + 1) * LANES] = value

            @pl.when(k == 1)
            def _():
                pltpu.make_async_copy(send.at[me], recv.at[me], own_sem.at[index]).start()

            @pl.when(k > 1)
            def _():
                remote(lax.rem(me + k - 1, devices)).start()

            return carry

        lax.fori_loop(0, devices, one, 0)
        remote(lax.rem(me + devices - 1, devices)).start()

    def await_group(recv, index):
        others = recv.at[pl.ds(0, devices - 1)]
        pltpu.make_async_copy(others, others, recv_sem.at[index]).wait()
        pltpu.make_async_copy(recv.at[0], recv.at[0], own_sem.at[index]).wait()

    for index, group in enumerate(leaders):
        transform(group, starts[index])
        if index == 0:
            pl.semaphore_wait(barrier, devices - 1)
        pack_and_send(group, send_lead[index], recv_lead[index], index)
    if not leaders:
        pl.semaphore_wait(barrier, devices - 1)

    def middle_step(step, carry):
        transform(middle, starts[lead] + step * middle.size)
        pack_and_send(middle, send_middle.at[step], recv_middle.at[step], step + lead)
        return carry

    lax.fori_loop(0, count, middle_step, 0)

    def make_table(group, start):
        rows = group.rows
        depth = devices * rows
        slot = lax.rem(lax.broadcasted_iota(jnp.int32, (rows, LANES), 0) // PARTS, group.size)

        def fill(device, carry):
            tile = jnp.zeros((rows, LANES), jnp.int32)
            for inner in range(group.size):
                tile = jnp.where(slot == inner, waves_ref[device * slots + start + inner], tile)
            wave[pl.ds(pl.multiple_of(device * rows, SUBLANES), rows), :] = tile.astype(jnp.float32)
            return carry

        lax.fori_loop(0, devices, fill, 0)
        waves = wave[:depth, :]
        lane = lax.broadcasted_iota(jnp.int32, (depth, LANES), 1).astype(jnp.float32)
        row = lax.broadcasted_iota(jnp.int32, (depth, LANES), 0)

        def angle(steps):
            turns = jnp.floor(steps * (1.0 / length))
            return (steps - turns * length) * (TWO_PI / length)

        base = angle(waves * lane) + jnp.where(lax.rem(row, PARTS) == 0, 0.0, TWO_PI / 4)
        weight = jnp.where(waves == 0.0, 1.0, 2.0)
        cosine, sine = weight * jnp.cos(base), weight * jnp.sin(base)
        stride = angle(waves * float(LANES))
        step_cosine, step_sine = jnp.cos(stride), jnp.sin(stride)
        for block in range(length // LANES):
            if block:
                cosine, sine = cosine * step_cosine - sine * step_sine, sine * step_cosine + cosine * step_sine
            high, low = split(cosine)
            span = slice(block * LANES, (block + 1) * LANES)
            table[:depth, span] = high
            table[depth : 2 * depth, span] = high
            table[2 * depth : 3 * depth, span] = low

    def synthesis(group, recv, index):
        depth = devices * group.rows
        await_group(recv, index)
        turn_block(recv, group, turned, left, lat_dev, members)
        values = left[:, :, : 2 * depth].reshape(lat_dev * padded, 2 * depth).astype(jnp.bfloat16)
        chunk = 2 * LANES

        def columns(n, carry):
            span = pl.ds(pl.multiple_of(n * chunk, chunk), chunk)
            total[:, :, span] += contract(values, table[: 3 * depth, span], depth).reshape(lat_dev, padded, chunk)
            return carry

        lax.fori_loop(0, length // chunk, columns, 0)

    left[...] = jnp.zeros_like(left)
    total[...] = jnp.zeros_like(total)
    for index, group in enumerate(leaders):
        make_table(group, starts[index])
        synthesis(group, recv_lead[index], index)

    def middle_synthesis(step, carry):
        make_table(middle, starts[lead] + step * middle.size)

        @pl.when(step < count - 1)
        def _():
            synthesis(middle, recv_middle.at[step], step + lead)

        return carry

    lax.fori_loop(0, count, middle_synthesis, 0)

    def sent(block, index):
        others = block.at[pl.ds(0, devices - 1)]
        pltpu.make_async_copy(others, others, send_sem.at[index]).wait()

    for index in range(lead):
        sent(send_lead[index], index)

    def middle_sent(step, carry):
        sent(send_middle.at[step], step + lead)
        return carry

    lax.fori_loop(0, count, middle_sent, 0)
    await_group(recv_middle.at[count - 1], lead + count - 1)


def exchange(old, noise, legendre, decay, amplitude, waves, lat_order, length):
    devices = lax.axis_size("lat") * lax.axis_size("lon")
    slots, scales, members, parts, width = old.shape
    lats = legendre.shape[1]
    lat_dev = lats // devices
    leaders, middle, count = plan(slots, lat_dev, members)
    groups = leaders + [middle]
    lead_blocks = tuple(pltpu.VMEM(group.block(devices), jnp.float32) for group in leaders)
    padded = round_up(members, SUBLANES)
    rows = max(group.rows for group in groups)
    depth = devices * rows
    vmem = pl.BlockSpec(memory_space=pltpu.VMEM)
    hbm = pl.BlockSpec(memory_space=pltpu.HBM)
    operands = (lat_order, waves, decay, amplitude, old, noise, legendre)
    operands = [pltpu.with_memory_space_constraint(array, pltpu.HBM) for array in operands]
    return pl.pallas_call(
        functools.partial(exchange_kernel, leaders, middle, count, members),
        in_specs=[hbm] * len(operands),
        out_specs=[vmem] * (scales + 3),
        out_shape=[pltpu.VMEM((slots, members, parts, width), jnp.float32)] * scales
        + [
            pltpu.VMEM((lat_dev, padded, length), jnp.float32),
            pltpu.VMEM((count,) + middle.block(devices), jnp.float32),
            pltpu.VMEM((3 * depth, length), jnp.bfloat16),
        ],
        scratch_shapes=[
            pltpu.SMEM(lat_order.shape, jnp.int32),
            pltpu.SMEM(waves.shape, jnp.int32),
            pltpu.SMEM(decay.shape, jnp.float32),
            pltpu.VMEM(amplitude.shape, jnp.float32),
            pltpu.SemaphoreType.DMA((4,)),
            pltpu.VMEM((2, scales, members, parts, width), jnp.float32),
            pltpu.VMEM((2, scales, members, parts, width), jnp.bfloat16),
            pltpu.VMEM((2, lats, width), jnp.float32),
            pltpu.VMEM((SUBLANES, width), jnp.float32),
            pltpu.VMEM((SUBLANES, width), jnp.float32),
            pltpu.VMEM((LANES, width), jnp.float32),
            pltpu.VMEM((lats, rows, LANES), jnp.float32),
            lead_blocks,
            lead_blocks,
            pltpu.VMEM((count,) + middle.block(devices), jnp.float32),
            pltpu.VMEM((depth, LANES), jnp.float32),
            pltpu.VMEM((max(group.wide for group in groups), depth), jnp.float32),
            pltpu.VMEM((lat_dev, padded, 2 * depth), jnp.float32),
            pltpu.SemaphoreType.DMA((3, 2)),
            pltpu.SemaphoreType.DMA((len(leaders) + count,)),
            pltpu.SemaphoreType.DMA((len(leaders) + count,)),
            pltpu.SemaphoreType.DMA((len(leaders) + count,)),
        ],
        compiler_params=pltpu.CompilerParams(collective_id=0, has_side_effects=True, vmem_limit_bytes=VMEM_LIMIT),
        name="exchange",
    )(*operands)


def finish_kernel(group, members, scales, *refs):
    new = refs[:scales]
    sum_ref, arrived_ref, table_ref, out_ref, new_out, turned, left, copy_sem = refs[scales:]
    lat_dev, padded, length = sum_ref.shape
    chunk = out_ref.shape[2]
    depth = left.shape[2] // 2
    step = pl.program_id(0)

    slots = new_out.shape[0]
    share = -(-slots // (length // chunk - 1))

    def write(slot, carry):
        for scale, ref in enumerate(new):
            pltpu.make_async_copy(ref.at[slot], new_out.at[slot, scale], copy_sem.at[scale]).start()
        return carry

    lax.fori_loop(jnp.minimum(share * step, slots), jnp.minimum(share * (step + 1), slots), write, 0)

    @pl.when(step == 0)
    def _():
        left[...] = jnp.zeros_like(left)
        turn_block(arrived_ref.at[arrived_ref.shape[0] - 1], group, turned, left, lat_dev, members)

    span = pl.ds(pl.multiple_of(step * chunk, chunk), chunk)
    values = left[...].reshape(lat_dev * padded, 2 * depth).astype(jnp.bfloat16)
    part = sum_ref[:, :, span] + contract(values, table_ref[: 3 * depth, span], depth).reshape(lat_dev, padded, chunk)
    out_ref[...] = part[:, :members, :]

    @pl.when(step == pl.num_programs(0) - 1)
    def _():
        for scale, ref in enumerate(new):
            pltpu.make_async_copy(ref, new_out.at[:, scale], copy_sem.at[scale]).wait()


def finish(new, summed, arrived, table):
    lat_dev, padded, length = summed.shape
    scales = len(new)
    slots, members, parts, width = new[0].shape
    group = plan(slots, lat_dev, members)[1]
    _, devices, rows, wide = arrived.shape
    depth = devices * rows
    chunk = 2 * LANES
    vmem = pl.BlockSpec(memory_space=pltpu.VMEM)
    return pl.pallas_call(
        functools.partial(finish_kernel, group, members, scales),
        grid=(length // chunk,),
        in_specs=[vmem] * (scales + 3),
        out_specs=[pl.BlockSpec((lat_dev, members, chunk), lambda n: (0, 0, n)), pl.BlockSpec(memory_space=pl.ANY)],
        out_shape=[
            jax.ShapeDtypeStruct((lat_dev, members, length), jnp.float32),
            jax.ShapeDtypeStruct((slots, scales, members, parts, width), jnp.float32),
        ],
        scratch_shapes=[
            pltpu.VMEM((wide, depth), jnp.float32),
            pltpu.VMEM((lat_dev, padded, 2 * depth), jnp.float32),
            pltpu.SemaphoreType.DMA((scales,)),
        ],
        compiler_params=pltpu.CompilerParams(dimension_semantics=("arbitrary",), vmem_limit_bytes=FINISH_LIMIT),
        name="finish",
    )(*[pltpu.with_memory_space_constraint(array, pltpu.VMEM) for array in (*new, summed, arrived, table)])


def local(coeffs_old, noise, legendre, decay, amplitude, wavenumber_of_slot, lat_order):
    slots, parts, scales, members, width = coeffs_old.shape
    length = 2 * legendre.shape[1]
    turn = (0, 2, 3, 1, 4)
    *new, summed, arrived, table = exchange(
        coeffs_old.transpose(turn), noise.transpose(turn), legendre, decay, amplitude, wavenumber_of_slot, lat_order, length
    )
    pattern, new = finish(new, summed, arrived, table)
    coeffs_new = new.transpose(0, 3, 1, 2, 4)
    return (coeffs_new, pattern)


def solution(mesh):
    split_rows = ("lat", "lon")
    in_specs = (
        P(split_rows, None, None, None, None),
        P(split_rows, None, None, None, None),
        P(split_rows, None, None),
        P(),
        P(),
        P(),
        P(),
    )
    out_specs = (P(split_rows, None, None, None, None), P(split_rows, None, None))
    return jax.shard_map(local, mesh=mesh, in_specs=in_specs, out_specs=out_specs, check_vma=False)
```
